8 devices in a mesh: ep: 4 (over z, y, x), dp: 2 (over core).
Axes of the slice: x: 2, y: 2, z: 1, core: 2. Of those that a mesh axis runs over, the one named last changes fastest.
Arguments:
- tokens: bfloat16 [4096, 256], P(('dp', 'ep'))
- dy_out: bfloat16 [4096, 256], P(('dp', 'ep'))
- dense_w1: bfloat16 [256, 256], replicated
- route_idx1: int32 [4096, 2], P(('dp', 'ep'))
- route_gate1: float32 [4096, 2], P(('dp', 'ep'))
- w_gate1: bfloat16 [8, 256, 896], P('ep')
- w_up1: bfloat16 [8, 256, 896], P('ep')
- w_down1: bfloat16 [8, 896, 256], P('ep')
- dense_w2: bfloat16 [256, 256], replicated
- route_idx2: int32 [4096, 2], P(('dp', 'ep'))
- route_gate2: float32 [4096, 2], P(('dp', 'ep'))
- w_gate2: bfloat16 [8, 256, 896], P('ep')
- w_up2: bfloat16 [8, 256, 896], P('ep')
- w_down2: bfloat16 [8, 896, 256], P('ep')
Outputs:
- output 1: bfloat16 [4096, 256], P(('dp', 'ep'))
- output 2: bfloat16 [256, 256], P(('dp', 'ep'))
- output 3: bfloat16 [8, 256, 896], P('ep', 'dp')
- output 4: bfloat16 [8, 256, 896], P('ep', 'dp')
- output 5: bfloat16 [8, 896, 256], P('ep', None, 'dp')
- output 6: bfloat16 [256, 256], P(('dp', 'ep'))
- output 7: bfloat16 [8, 256, 896], P('ep', 'dp')
- output 8: bfloat16 [8, 256, 896], P('ep', 'dp')
- output 9: bfloat16 [8, 896, 256], P('ep', None, 'dp')
All inputs are finite; a program needn't handle non-finite values.
Results may differ from the reference program's by a relative error of at most 0.02.
Values are sent between devices in bfloat16 or wider.
A program may use at most 1 GiB of HBM per device.

```python
import jax
import jax.numpy as jnp

TOK = 512
D = 256
FF = 896
EXPERTS = 8
TOP = 2
SOURCES = 8
BASE = TOK * TOP // EXPERTS
CAPACITY = 2 * BASE


def draw_routing(key):
    key_tok, key_exp, key_shift = jax.random.split(key, 3)
    tok_order = jax.vmap(lambda src_key: jax.random.permutation(src_key, TOK))(jax.random.split(key_tok, SOURCES))
    exp_order = jax.vmap(lambda src_key: jax.random.permutation(src_key, EXPERTS))(jax.random.split(key_exp, SOURCES))
    shift = jax.random.randint(key_shift, (SOURCES, EXPERTS // 2), 0, BASE // 2 + 1, dtype=jnp.int32)
    shift = shift.at[:, 0].set(BASE)
    sizes = jnp.stack([BASE + shift, BASE - shift], axis=2).reshape(SOURCES, EXPERTS)
    block_end = jnp.cumsum(sizes, axis=1, dtype=jnp.int32)
    place = jnp.arange(TOP, dtype=jnp.int32)[None, None, :] * TOK + tok_order[:, :, None].astype(jnp.int32)
    block = jax.vmap(lambda end_row, place_row: jnp.searchsorted(end_row, place_row, side='right'))(block_end, place)
    expert = jnp.take_along_axis(exp_order, block.reshape(SOURCES, TOK * TOP), axis=1)
    return expert.reshape(SOURCES * TOK, TOP).astype(jnp.int32)


def setup_inputs(seed: int = 0) -> dict:
    keys = jax.random.split(jax.random.key(seed), 14)
    n_all = SOURCES * TOK

    def normal(key, shape, scale):
        return (scale * jax.random.normal(key, shape, jnp.float32)).astype(jnp.bfloat16)

    def gates(key):
        return jax.random.uniform(key, (n_all, TOP), jnp.float32, 0.5, 1.5) * TOP ** -0.5

    return {
        'tokens': normal(keys[0], (n_all, D), 1.0),
        'dy_out': normal(keys[1], (n_all, D), 1.0),
        'dense_w1': normal(keys[2], (D, D), 0.5 * D ** -0.5),
        'route_idx1': draw_routing(keys[3]),
        'route_gate1': gates(keys[4]),
        'w_gate1': normal(keys[5], (EXPERTS, D, FF), D ** -0.5),
        'w_up1': normal(keys[6], (EXPERTS, D, FF), D ** -0.5),
        'w_down1': normal(keys[7], (EXPERTS, FF, D), FF ** -0.5),
        'dense_w2': normal(keys[8], (D, D), 0.5 * D ** -0.5),
        'route_idx2': draw_routing(keys[9]),
        'route_gate2': gates(keys[10]),
        'w_gate2': normal(keys[11], (EXPERTS, D, FF), D ** -0.5),
        'w_up2': normal(keys[12], (EXPERTS, D, FF), D ** -0.5),
        'w_down2': normal(keys[13], (EXPERTS, FF, D), FF ** -0.5),
    }


def group_rows(route_idx, n_rows):
    flat_exp = route_idx.reshape(-1)
    n_copies = flat_exp.shape[0]
    order = jnp.argsort(flat_exp, stable=True).astype(jnp.int32)
    sorted_exp = jnp.take(flat_exp, order)
    counts = jnp.zeros((EXPERTS,), jnp.int32).at[flat_exp].add(1)
    starts = jnp.cumsum(counts, dtype=jnp.int32) - counts
    dest_row = (sorted_exp * n_rows + jnp.arange(n_copies, dtype=jnp.int32) - jnp.take(starts, sorted_exp)).astype(jnp.int32)
    return jnp.zeros((n_copies,), jnp.int32).at[order].set(dest_row).reshape(route_idx.shape)


def moe_layer(x_tok, dense_w, route_idx, route_gate, w_gate, w_up, w_down):
    n_all = x_tok.shape[0]
    n_rows = SOURCES * CAPACITY
    x_wide = x_tok.astype(jnp.float32)
    mixed = (x_wide + jnp.dot(x_wide, dense_w.astype(jnp.float32), preferred_element_type=jnp.float32)).astype(jnp.bfloat16)
    flat_pos = group_rows(route_idx, n_rows)
    tok_ids = jnp.broadcast_to(jnp.arange(n_all, dtype=jnp.int32)[:, None], route_idx.shape)
    row_tok = jnp.full((EXPERTS * n_rows,), n_all, jnp.int32).at[flat_pos.reshape(-1)].set(tok_ids.reshape(-1))
    buffer = jnp.take(mixed, row_tok, axis=0, mode='fill', fill_value=0).reshape(EXPERTS, n_rows, D).astype(jnp.float32)
    a_pre = jnp.einsum('erd,edf->erf', buffer, w_gate.astype(jnp.float32))
    b_pre = jnp.einsum('erd,edf->erf', buffer, w_up.astype(jnp.float32))
    hidden = (jax.nn.silu(a_pre) * b_pre).astype(jnp.bfloat16)
    expert_out = jnp.einsum('erf,efd->erd', hidden.astype(jnp.float32), w_down.astype(jnp.float32)).astype(jnp.bfloat16)
    picked = jnp.take(expert_out.reshape(EXPERTS * n_rows, D), flat_pos, axis=0).astype(jnp.float32)
    return (mixed.astype(jnp.float32) + jnp.sum(route_gate[:, :, None] * picked, axis=1)).astype(jnp.bfloat16)


def reference(tokens, dy_out, dense_w1, route_idx1, route_gate1, w_gate1, w_up1, w_down1, dense_w2, route_idx2, route_gate2, w_gate2, w_up2, w_down2):
    def forward(x_tok, dense_a, gate_a, up_a, down_a, dense_b, gate_b, up_b, down_b):
        mid_tok = moe_layer(x_tok, dense_a, route_idx1, route_gate1, gate_a, up_a, down_a)
        return moe_layer(mid_tok, dense_b, route_idx2, route_gate2, gate_b, up_b, down_b)

    y_out, pullback = jax.vjp(forward, tokens, dense_w1, w_gate1, w_up1, w_down1, dense_w2, w_gate2, w_up2, w_down2)
    (grad_tok, grad_dense1, grad_gate1, grad_up1, grad_down1, grad_dense2, grad_gate2, grad_up2, grad_down2) = pullback(dy_out)
    return (grad_tok, grad_dense1, grad_gate1, grad_up1, grad_down1, grad_dense2, grad_gate2, grad_up2, grad_down2)
```

```python
import functools

import jax
import jax.numpy as jnp
from jax import lax
from jax.experimental import pallas as pl
from jax.experimental.pallas import tpu as pltpu
from jax.sharding import PartitionSpec as P

MESH = pl.DeviceIdType.MESH
BF = jnp.bfloat16
F32 = jnp.float32
NN = ((1,), (0,))
NT = ((1,), (1,))
TN = ((0,), (0,))
EP = 4
DP = 2
E_LOC = 2
TOK = 512
CAP = 256
D = 256
FF = 896
ROUTE, X_IN, O_ONE, DY, Y_ONE, GR_TWO, GM, GR_ONE = range(8)


def dot(a, b, dims=NN):
    return lax.dot_general(a, b, (dims, ((), ())), preferred_element_type=F32)


def place(k):
    return k + 3 * ((k + 3) // 4)


def onehot(key_row):
    rows = lax.broadcasted_iota(jnp.int32, (CAP, TOK), 0)
    return jnp.where(rows == key_row, 1.0, 0.0).astype(BF)


def gate_column(key_row, gate_row):
    rows = lax.broadcasted_iota(jnp.int32, (CAP, TOK), 0)
    return jnp.sum(jnp.where(rows == key_row, gate_row, 0.0), axis=1, keepdims=True)


def kernel(tokens, dy, route, m1, g1, u1, w1, m2, g2, u2, w2,
           dx_out, gd1, gg1, gu1, gw1, gd2, gg2, gu2, gw2,
           rt, xin, dyb, yb, gmb, oret, grt2, grt1,
           vm1, vg1, vu1, vw1, vm2, vg2, vu2, vw2,
           tri, keys, gates, keyj, x1, x2, gout, a1, b1, hb, ga, gb, u_home, p0, p1,
           wg, wu, wd, rg, ru, rd, dpart, drecv, dxb,
           loc_sem, ep_send, ep_recv, dp_send, dp_recv, all_send, all_recv, out_sem):
    me = lax.axis_index('ep')
    dp = lax.axis_index('dp')
    flat = dp * EP + me
    other = 1 - dp

    def partner(k):
        return (me // 2 + k // 2) % 2 * 2 + (me + k) % 2

    loads = [(route, rt.at[0]), (tokens, xin.at[0]), (dy, dyb.at[0]), (m1, vm1), (g1, vg1), (u1, vu1), (w1, vw1),
             (m2, vm2), (g2, vg2), (u2, vu2), (w2, vw2)]
    loads = [pltpu.make_async_copy(src, dst, loc_sem.at[n]) for n, (src, dst) in enumerate(loads)]
    for copy in loads:
        copy.start()

    barrier = pltpu.get_barrier_semaphore()
    for r in range(1, EP * DP):
        peer = (flat + r) % (EP * DP)
        pl.semaphore_signal(barrier, inc=1, device_id={'ep': peer % EP, 'dp': peer // EP}, device_id_type=MESH)
    pl.semaphore_wait(barrier, EP * DP - 1)

    def exchange(phase, k, src, dst):
        return pltpu.make_async_remote_copy(src_ref=src, dst_ref=dst, send_sem=ep_send.at[phase, k], recv_sem=ep_recv.at[phase, k],
                                            device_id={'ep': partner(k)}, device_id_type=MESH)

    def spread(phase, buf, k):
        return exchange(phase, k, buf.at[0], buf.at[k])

    def giveback(phase, buf, k):
        return exchange(phase, k, buf.at[k], buf.at[k + 3])

    loads[0].wait()
    for k in range(1, EP):
        spread(ROUTE, rt, k).start()
    loads[1].wait()
    for k in range(1, EP):
        spread(X_IN, xin, k).start()

    tri[...] = jnp.where(lax.broadcasted_iota(jnp.int32, (TOK, TOK), 0) < lax.broadcasted_iota(jnp.int32, (TOK, TOK), 1), 1.0, 0.0).astype(BF)
    expert = lax.broadcasted_iota(jnp.int32, (E_LOC * EP, TOK), 0).astype(F32)

    def make_keys(k):
        info = rt[k]
        for l in range(2):
            hit0 = info[2 * l:2 * l + 1] == expert
            hit1 = info[2 * l + 1:2 * l + 2] == expert
            both = jnp.where(hit0, 1.0, jnp.where(hit1, 1.0, 0.0))
            rank = dot(both.astype(BF), tri[...]).astype(jnp.int32)
            keys[l, k] = jnp.where(both > 0.5, rank, -1)
            gates[l, k] = jnp.where(hit0, info[4 + 2 * l:5 + 2 * l], jnp.where(hit1, info[5 + 2 * l:6 + 2 * l], 0.0))
        return info

    info = make_keys(0)
    for j in range(2):
        keyj[j] = jnp.where(info[j:j + 1] == expert, keys[0, 0], -1)
    for copy in loads[2:]:
        copy.wait()

    def mixed(x, m):
        return (x.astype(F32) + dot(x, m[...])).astype(BF)

    def forward_one(k, carry):
        @pl.when(k > 0)
        def _():
            spread(ROUTE, rt, k).wait_recv()
            make_keys(k)
            spread(X_IN, xin, k).wait_recv()

        u = mixed(xin[k], vm1)

        @pl.when(k == 0)
        def _():
            u_home[...] = u

        def one(el, c):
            rows = pl.ds(pl.multiple_of(k * CAP, CAP), CAP)
            key = keys[0, k, pl.ds(me * E_LOC + el, 1), :]
            x = dot(onehot(key), u).astype(BF)
            x1[el, rows] = x
            a = dot(x, vg1[el])
            b = dot(x, vu1[el])
            a1[el, rows] = a
            b1[el, rows] = b
            h = (a * (0.5 * jnp.tanh(0.5 * a) + 0.5) * b).astype(BF)
            oret[k, pl.ds(pl.multiple_of(el * CAP, CAP), CAP)] = dot(h, vw1[el]).astype(BF)
            return c

        lax.fori_loop(0, E_LOC, one, 0)

        @pl.when(k > 0)
        def _():
            giveback(O_ONE, oret, k).start()
        return carry

    lax.fori_loop(0, EP, forward_one, 0)
    for k in range(1, EP):
        spread(DY, dyb, k).start()

    p0[...] = jnp.zeros_like(p0)
    p1[...] = jnp.zeros_like(p1)

    def combine_one(k, carry):
        @pl.when(k > 0)
        def _():
            giveback(O_ONE, oret, k).wait_recv()

        def one(el, c):
            rows = oret[place(k), pl.ds(pl.multiple_of(el * CAP, CAP), CAP)]
            e = partner(k) * E_LOC + el
            p0[...] += dot(onehot(keyj[0, pl.ds(e, 1), :]), rows, TN)
            p1[...] += dot(onehot(keyj[1, pl.ds(e, 1), :]), rows, TN)
            return c

        lax.fori_loop(0, E_LOC, one, 0)
        return carry

    lax.fori_loop(0, EP, combine_one, 0)
    gate0 = jnp.transpose(jnp.broadcast_to(rt[0, 4:5], (8, TOK)))[:, :1]
    gate1 = jnp.transpose(jnp.broadcast_to(rt[0, 5:6], (8, TOK)))[:, :1]
    yb[0] = (u_home[...].astype(F32) + (gate0 * p0[...] + gate1 * p1[...])).astype(BF)
    for k in range(1, EP):
        spread(Y_ONE, yb, k).start()

    def expert_backward(k, el, x_rows, a, b, vg, vu, vw, ret):
        rows = pl.ds(pl.multiple_of(k * CAP, CAP), CAP)
        dh = dot(gout[el, rows], vw[el], NT).astype(BF).astype(F32)
        sig = 0.5 * jnp.tanh(0.5 * a) + 0.5
        s = a * sig
        hb[el, rows] = (s * b).astype(BF)
        grad_a = (dh * b * (sig + s * (1.0 - sig))).astype(BF)
        grad_b = (dh * s).astype(BF)
        ga[el, rows] = grad_a
        gb[el, rows] = grad_b
        back = dot(grad_a, vg[el], NT) + dot(grad_b, vu[el], NT)
        ret[k, pl.ds(pl.multiple_of(el * CAP, CAP), CAP)] = back.astype(BF)

    def layer_two(k, carry):
        @pl.when(k > 0)
        def _():
            spread(Y_ONE, yb, k).wait_recv()
            spread(DY, dyb, k).wait_recv()

        u = mixed(yb[k], vm2)

        def one(el, c):
            rows = pl.ds(pl.multiple_of(k * CAP, CAP), CAP)
            e = pl.ds(me * E_LOC + el, 1)
            key = keys[1, k, e, :]
            pick = onehot(key)
            x = dot(pick, u).astype(BF)
            x2[el, rows] = x
            gout[el, rows] = (dot(pick, dyb[k]) * gate_column(key, gates[1, k, e, :])).astype(BF)
            a = dot(x, vg2[el])
            b = dot(x, vu2[el])
            expert_backward(k, el, x, a, b, vg2, vu2, vw2, grt2)
            return c

        lax.fori_loop(0, E_LOC, one, 0)

        @pl.when(k > 0)
        def _():
            giveback(GR_TWO, grt2, k).start()
        return carry

    lax.fori_loop(0, EP, layer_two, 0)

    def pair(l, n, src, dst):
        return pltpu.make_async_remote_copy(src_ref=src, dst_ref=dst, send_sem=dp_send.at[l, n], recv_sem=dp_recv.at[l, n],
                                            device_id={'dp': other}, device_id_type=MESH)

    def pairs(l):
        return [pair(l, n, part.at[l, other], got.at[l]) for n, (part, got) in enumerate(((wg, rg), (wu, ru), (wd, rd)))]

    def weight_grads(l, x_all):
        half = D // DP

        def one(el, c):
            x = x_all[el]
            go = gout[el]
            down = dot(hb[el], go, TN).astype(BF)
            gate = dot(x, ga[el], TN).astype(BF)
            up = dot(x, gb[el], TN).astype(BF)
            for d in range(DP):
                wd[l, d, el] = down[:, d * half:(d + 1) * half]
                wg[l, d, el] = gate[d * half:(d + 1) * half]
                wu[l, d, el] = up[d * half:(d + 1) * half]
            return c

        lax.fori_loop(0, E_LOC, one, 0)
        for copy in pairs(l):
            copy.start()

    weight_grads(1, x2)

    def backward_combine(l, phase, ret, grad_y):
        p0[...] = jnp.zeros_like(p0)

        def step(k, carry):
            @pl.when(k > 0)
            def _():
                giveback(phase, ret, k).wait_recv()

            def one(el, c):
                rows = ret[place(k), pl.ds(pl.multiple_of(el * CAP, CAP), CAP)]
                e = partner(k) * E_LOC + el
                p0[...] += dot(onehot(keys[l, 0, pl.ds(e, 1), :]), rows, TN)
                return c

            lax.fori_loop(0, E_LOC, one, 0)
            return carry

        lax.fori_loop(0, EP, step, 0)
        return (grad_y.astype(F32) + p0[...]).astype(BF)

    def grad_input(grad_mixed, m):
        return (grad_mixed.astype(F32) + dot(grad_mixed, m[...], NT)).astype(BF)

    def dense_copies(l):
        copies = []
        for r in range(1, EP * DP):
            peer = (flat + r) % (EP * DP)
            copies.append(pltpu.make_async_remote_copy(
                src_ref=dpart.at[l, peer], dst_ref=drecv.at[l, r], send_sem=all_send.at[l, r], recv_sem=all_recv.at[l, r],
                device_id={'ep': peer % EP, 'dp': peer // EP}, device_id_type=MESH))
        return copies

    def dense_grad(l, x, grad_mixed):
        part = dot(x, grad_mixed, TN).astype(BF)
        for q in range(EP * DP):
            dpart[l, q] = part[q * 32:(q + 1) * 32]
        for copy in dense_copies(l):
            copy.start()

    grad_mixed = backward_combine(1, GR_TWO, grt2, dyb[0])
    gmb[0] = grad_input(grad_mixed, vm2)
    for k in range(1, EP):
        spread(GM, gmb, k).start()
    dense_grad(1, yb[0], grad_mixed)

    def backward_one(k, carry):
        @pl.when(k > 0)
        def _():
            spread(GM, gmb, k).wait_recv()

        def one(el, c):
            rows = pl.ds(pl.multiple_of(k * CAP, CAP), CAP)
            e = pl.ds(me * E_LOC + el, 1)
            key = keys[0, k, e, :]
            gout[el, rows] = (dot(onehot(key), gmb[k]) * gate_column(key, gates[0, k, e, :])).astype(BF)
            expert_backward(k, el, x1[el, rows], a1[el, rows], b1[el, rows], vg1, vu1, vw1, grt1)
            return c

        lax.fori_loop(0, E_LOC, one, 0)

        @pl.when(k > 0)
        def _():
            giveback(GR_ONE, grt1, k).start()
        return carry

    lax.fori_loop(0, EP, backward_one, 0)
    weight_grads(0, x1)

    outs = []

    def emit(src, dst):
        copy = pltpu.make_async_copy(src, dst, out_sem.at[len(outs)])
        copy.start()
        outs.append(copy)

    def finish(l, gate_out, up_out, down_out):
        for copy, part, got, out in zip(pairs(l), (wg, wu, wd), (rg, ru, rd), (gate_out, up_out, down_out)):
            copy.wait_recv()
            got[l] = (part[l, dp].astype(F32) + got[l].astype(F32)).astype(BF)
            emit(got.at[l], out)

    def finish_dense(l, out):
        total = dpart[l, flat].astype(F32)
        for r, copy in enumerate(dense_copies(l), 1):
            copy.wait_recv()
            total += drecv[l, r].astype(F32)
        drecv[l, 0] = total.astype(BF)
        emit(drecv.at[l, 0], out)

    finish(1, gg2, gu2, gw2)
    finish_dense(1, gd2)
    grad_mixed = backward_combine(0, GR_ONE, grt1, gmb[0])
    dense_grad(0, xin[0], grad_mixed)
    dxb[...] = grad_input(grad_mixed, vm1)
    emit(dxb, dx_out)
    finish(0, gg1, gu1, gw1)
    finish_dense(0, gd1)

    for k in range(1, EP):
        for phase, buf in ((ROUTE, rt), (X_IN, xin), (DY, dyb), (Y_ONE, yb), (GM, gmb)):
            spread(phase, buf, k).wait_send()
        for phase, buf in ((O_ONE, oret), (GR_TWO, grt2), (GR_ONE, grt1)):
            giveback(phase, buf, k).wait_send()
    for l in range(2):
        for copy in pairs(l) + dense_copies(l):
            copy.wait_send()
    for copy in outs:
        copy.wait()


def solution(mesh):
    tok_spec = P(('dp', 'ep'), None)
    exp_spec = P('ep', None, None)
    layer_specs = (P(None, None), tok_spec, tok_spec, exp_spec, exp_spec, exp_spec)
    grad_specs = (P(('dp', 'ep'), None), P('ep', 'dp', None), P('ep', 'dp', None), P('ep', None, 'dp'))

    def local_step(tokens, dy_out, dense_w1, route_idx1, route_gate1, w_gate1, w_up1, w_down1, dense_w2, route_idx2, route_gate2, w_gate2, w_up2, w_down2):
        route = jnp.concatenate([route_idx1.astype(F32).T, route_idx2.astype(F32).T, route_gate1.T, route_gate2.T], axis=0)
        hbm = pl.BlockSpec(memory_space=pl.ANY)
        half = D // DP

        def sds(*shape):
            return jax.ShapeDtypeStruct(shape, BF)

        grads = (sds(32, D), sds(E_LOC, half, FF), sds(E_LOC, half, FF), sds(E_LOC, FF, half))
        vm = pltpu.VMEM
        dma = pltpu.SemaphoreType.DMA
        weights = [vm((D, D), BF), vm((E_LOC, D, FF), BF), vm((E_LOC, D, FF), BF), vm((E_LOC, FF, D), BF)]
        spread_buf = vm((EP, TOK, D), BF)
        ret_buf = vm((2 * EP - 1, TOK, D), BF)
        scratch = [vm((EP, 8, TOK), F32), spread_buf, spread_buf, spread_buf, spread_buf, ret_buf, ret_buf, ret_buf]
        scratch += weights + weights
        scratch += [vm((TOK, TOK), BF), vm((2, EP, 8, TOK), jnp.int32), vm((2, EP, 8, TOK), F32), vm((2, 8, TOK), jnp.int32)]
        scratch += [vm((E_LOC, EP * CAP, D), BF)] * 3
        scratch += [vm((E_LOC, EP * CAP, FF), F32)] * 2
        scratch += [vm((E_LOC, EP * CAP, FF), BF)] * 3
        scratch += [vm((TOK, D), BF), vm((TOK, D), F32), vm((TOK, D), F32)]
        scratch += [vm((2, DP, E_LOC, half, FF), BF)] * 2 + [vm((2, DP, E_LOC, FF, half), BF)]
        scratch += [vm((2, E_LOC, half, FF), BF)] * 2 + [vm((2, E_LOC, FF, half), BF)]
        scratch += [vm((2, EP * DP, 32, D), BF), vm((2, EP * DP, 32, D), BF), vm((TOK, D), BF)]
        scratch += [dma((11,)), dma((8, EP)), dma((8, EP)), dma((2, 3)), dma((2, 3)), dma((2, 8)), dma((2, 8)), dma((9,))]
        return pl.pallas_call(
            kernel,
            out_shape=(sds(TOK, D),) + grads + grads,
            in_specs=[hbm] * 11,
            out_specs=(hbm,) * 9,
            scratch_shapes=scratch,
            name='moe_backward',
            compiler_params=pltpu.CompilerParams(collective_id=0, has_side_effects=True, vmem_limit_bytes=67043328),
        )(tokens, dy_out, route, dense_w1, w_gate1, w_up1, w_down1, dense_w2, w_gate2, w_up2, w_down2)

    return jax.shard_map(local_step, mesh=mesh, in_specs=(tok_spec, tok_spec) + layer_specs + layer_specs,
                         out_specs=(tok_spec,) + grad_specs + grad_specs, check_vma=False)
```

```python
import jax
import jax.numpy as jnp
from jax import lax
from jax.experimental import pallas as pl
from jax.experimental.pallas import tpu as pltpu
from jax.sharding import PartitionSpec as P

MESH = pl.DeviceIdType.MESH
BF = jnp.bfloat16
F32 = jnp.float32
NN = ((1,), (0,))
NT = ((1,), (1,))
TN = ((0,), (0,))
EP = 4
DP = 2
E_LOC = 2
TOK = 512
CAP = 256
D = 256
FF = 896
X_IN, DY, Y_ONE, GM = range(4)
O_ONE, GR_TWO, GR_ONE = range(3)


def dot(a, b, dims=NN):
    return lax.dot_general(a, b, (dims, ((), ())), preferred_element_type=F32)


def place(k):
    return k + 3 * ((k + 3) // 4)


def onehot(key_row):
    rows = lax.broadcasted_iota(jnp.int32, (CAP, TOK), 0)
    return jnp.where(rows == key_row, 1.0, 0.0).astype(BF)


def gate_column(key_row, gate_row):
    rows = lax.broadcasted_iota(jnp.int32, (CAP, TOK), 0)
    return jnp.sum(jnp.where(rows == key_row, gate_row, 0.0), axis=1, keepdims=True)


def kernel(tokens, dy, idx1, idx2, gate1, gate2, m1, g1, u1, w1, m2, g2, u2, w2,
           dx_out, own_g, own_u, own_w, got_g, got_u, got_w, dense_out,
           ibuf, gbuf, rt, xin, dyb, yb, gmb, oret, grt2, grt1,
           vm1, vg1, vu1, vw1, vm2, vg2, vu2, vw2,
           tri, keys, gates, keyj, x1, x2, gout, a1, b1, hb, ga, gb, u_home, p0, p1,
           wg, wu, wd, dpart, dxb,
           loc_sem, rt_send, rt_recv, ag_send, ag_recv, ret_send, ret_recv, dp_send, dp_recv, all_send, all_recv, out_sem):
    me = lax.axis_index('ep')
    dp = lax.axis_index('dp')
    flat = dp * EP + me
    other = 1 - dp

    def partner(k):
        return (me // 2 + k // 2) % 2 * 2 + (me + k) % 2

    loads = [(idx1, ibuf.at[0]), (idx2, ibuf.at[1]), (gate1, gbuf.at[0]), (gate2, gbuf.at[1]), (tokens, xin.at[0]),
             (m1, vm1), (g1, vg1), (u1, vu1), (w1, vw1), (dy, dyb.at[0]), (m2, vm2), (g2, vg2), (u2, vu2), (w2, vw2)]
    loads = [pltpu.make_async_copy(src, dst, loc_sem.at[n]) for n, (src, dst) in enumerate(loads)]
    for copy in loads:
        copy.start()

    barrier = pltpu.get_barrier_semaphore()
    for r in range(1, EP * DP):
        peer = (flat + r) % (EP * DP)
        pl.semaphore_signal(barrier, inc=1, device_id={'ep': peer % EP, 'dp': peer // EP}, device_id_type=MESH)

    for copy in loads[:4]:
        copy.wait()
    rt[0] = jnp.concatenate([ibuf[0].astype(F32), ibuf[1].astype(F32), gbuf[0], gbuf[1]], axis=0)
    loads[4].wait()
    pl.semaphore_wait(barrier, EP * DP - 1)

    def remote(src, dst, send, recv, k):
        return pltpu.make_async_remote_copy(src_ref=src, dst_ref=dst, send_sem=send, recv_sem=recv,
                                            device_id={'ep': partner(k)}, device_id_type=MESH)

    def tell(k):
        return remote(rt.at[0], rt.at[k], rt_send.at[k], rt_recv.at[k], k)

    def half(h):
        return pl.ds(h * CAP, CAP)

    def ship(phase, buf, k, piece):
        rows = half(piece if k == 1 else 1 - piece)
        return remote(buf.at[0, rows], buf.at[k, rows], ag_send.at[phase, k, piece], ag_recv.at[phase, k, piece], k)

    def relay(phase, buf, via):
        rows = half(via - 1)
        return remote(buf.at[via, rows], buf.at[3, rows], ag_send.at[phase, 3, via - 1], ag_recv.at[phase, 3, via - 1], 3 - via)

    def spread(phase, buf):
        for piece in range(2):
            for k in (1, 2):
                ship(phase, buf, k, piece).start()

    def pass_on(phase, buf):
        for via in (1, 2):
            ship(phase, buf, via, 0).wait_recv()
            relay(phase, buf, via).start()

    def arrive(phase, buf, k):
        for near in (1, 2):
            @pl.when(k == near)
            def _():
                ship(phase, buf, near, 1).wait_recv()

        @pl.when(k == 3)
        def _():
            for via in (1, 2):
                relay(phase, buf, via).wait_recv()

    def giveback(phase, buf, k, el):
        rows = pl.ds(pl.multiple_of(el * CAP, CAP), CAP)
        return remote(buf.at[k, rows], buf.at[k + 3, rows], ret_send.at[phase, k, el], ret_recv.at[phase, k, el], k)

    for k in range(1, EP):
        tell(k).start()
    spread(X_IN, xin)

    tri[...] = jnp.where(lax.broadcasted_iota(jnp.int32, (TOK, TOK), 0) < lax.broadcasted_iota(jnp.int32, (TOK, TOK), 1), 1.0, 0.0).astype(BF)
    expert = lax.broadcasted_iota(jnp.int32, (E_LOC * EP, TOK), 0).astype(F32)

    def make_keys(k):
        info = rt[k]
        for l in range(2):
            hit0 = info[2 * l:2 * l + 1] == expert
            hit1 = info[2 * l + 1:2 * l + 2] == expert
            both = jnp.where(hit0, 1.0, jnp.where(hit1, 1.0, 0.0))
            rank = dot(both.astype(BF), tri[...]).astype(jnp.int32)
            keys[l, k] = jnp.where(both > 0.5, rank, -1)
            gates[l, k] = jnp.where(hit0, info[4 + 2 * l:5 + 2 * l], jnp.where(hit1, info[5 + 2 * l:6 + 2 * l], 0.0))
        return info

    info = make_keys(0)
    for j in range(2):
        keyj[j] = jnp.where(info[j:j + 1] == expert, keys[0, 0], -1)
    for copy in loads[5:9]:
        copy.wait()

    def mixed(x, m):
        return (x.astype(F32) + dot(x, m[...])).astype(BF)

    def forward_one(k, carry):
        @pl.when(k == 1)
        def _():
            pass_on(X_IN, xin)

        @pl.when(k > 0)
        def _():
            tell(k).wait_recv()
            make_keys(k)

        arrive(X_IN, xin, k)
        u = mixed(xin[k], vm1)

        @pl.when(k == 0)
        def _():
            u_home[...] = u

        def one(el, c):
            rows = pl.ds(pl.multiple_of(k * CAP, CAP), CAP)
            key = keys[0, k, pl.ds(me * E_LOC + el, 1), :]
            x = dot(onehot(key), u).astype(BF)
            x1[el, rows] = x
            a = dot(x, vg1[el])
            b = dot(x, vu1[el])
            a1[el, rows] = a
            b1[el, rows] = b
            h = (a * (0.5 * jnp.tanh(0.5 * a) + 0.5) * b).astype(BF)
            oret[k, pl.ds(pl.multiple_of(el * CAP, CAP), CAP)] = dot(h, vw1[el]).astype(BF)

            @pl.when(k > 0)
            def _():
                giveback(O_ONE, oret, k, el).start()
            return c

        lax.fori_loop(0, E_LOC, one, 0)
        return carry

    lax.fori_loop(0, EP, forward_one, 0)
    for copy in loads[9:]:
        copy.wait()
    spread(DY, dyb)

    p0[...] = jnp.zeros_like(p0)
    p1[...] = jnp.zeros_like(p1)

    def combine_one(k, carry):
        def one(el, c):
            @pl.when(k > 0)
            def _():
                giveback(O_ONE, oret, k, el).wait_recv()

            rows = oret[place(k), pl.ds(pl.multiple_of(el * CAP, CAP), CAP)]
            e = partner(k) * E_LOC + el
            p0[...] += dot(onehot(keyj[0, pl.ds(e, 1), :]), rows, TN)
            p1[...] += dot(onehot(keyj[1, pl.ds(e, 1), :]), rows, TN)
            return c

        lax.fori_loop(0, E_LOC, one, 0)
        return carry

    lax.fori_loop(0, EP, combine_one, 0)
    gcol0 = jnp.transpose(jnp.broadcast_to(rt[0, 4:5], (8, TOK)))[:, :1]
    gcol1 = jnp.transpose(jnp.broadcast_to(rt[0, 5:6], (8, TOK)))[:, :1]
    yb[0] = (u_home[...].astype(F32) + (gcol0 * p0[...] + gcol1 * p1[...])).astype(BF)
    spread(Y_ONE, yb)

    def expert_backward(k, el, a, b, vg, vu, vw, phase, ret):
        rows = pl.ds(pl.multiple_of(k * CAP, CAP), CAP)
        dh = dot(gout[el, rows], vw[el], NT).astype(BF).astype(F32)
        sig = 0.5 * jnp.tanh(0.5 * a) + 0.5
        s = a * sig
        hb[el, rows] = (s * b).astype(BF)
        grad_a = (dh * b * (sig + s * (1.0 - sig))).astype(BF)
        grad_b = (dh * s).astype(BF)
        ga[el, rows] = grad_a
        gb[el, rows] = grad_b
        back = dot(grad_a, vg[el], NT) + dot(grad_b, vu[el], NT)
        ret[k, pl.ds(pl.multiple_of(el * CAP, CAP), CAP)] = back.astype(BF)

        @pl.when(k > 0)
        def _():
            giveback(phase, ret, k, el).start()

    def layer_two(k, carry):
        @pl.when(k == 1)
        def _():
            pass_on(DY, dyb)
            pass_on(Y_ONE, yb)

        arrive(DY, dyb, k)
        arrive(Y_ONE, yb, k)
        u = mixed(yb[k], vm2)

        def one(el, c):
            rows = pl.ds(pl.multiple_of(k * CAP, CAP), CAP)
            e = pl.ds(me * E_LOC + el, 1)
            key = keys[1, k, e, :]
            pick = onehot(key)
            x = dot(pick, u).astype(BF)
            x2[el, rows] = x
            gout[el, rows] = (dot(pick, dyb[k]) * gate_column(key, gates[1, k, e, :])).astype(BF)
            a = dot(x, vg2[el])
            b = dot(x, vu2[el])
            expert_backward(k, el, a, b, vg2, vu2, vw2, GR_TWO, grt2)
            return c

        lax.fori_loop(0, E_LOC, one, 0)
        return carry

    lax.fori_loop(0, EP, layer_two, 0)

    stacks = ((wg, own_g, got_g), (wu, own_u, got_u), (wd, own_w, got_w))

    def pairs(l):
        return [pltpu.make_async_remote_copy(src_ref=part.at[l, other], dst_ref=got.at[l], send_sem=dp_send.at[l, n],
                                             recv_sem=dp_recv.at[l, n], device_id={'dp': other}, device_id_type=MESH)
                for n, (part, own, got) in enumerate(stacks)]

    outs = []

    def emit(src, dst):
        copy = pltpu.make_async_copy(src, dst, out_sem.at[len(outs)])
        copy.start()
        outs.append(copy)

    def weight_grads(l, x_all):
        half_d = D // DP

        def one(el, c):
            x = x_all[el]
            go = gout[el]
            down = dot(hb[el], go, TN).astype(BF)
            gate = dot(x, ga[el], TN).astype(BF)
            up = dot(x, gb[el], TN).astype(BF)
            for d in range(DP):
                wd[l, d, el] = down[:, d * half_d:(d + 1) * half_d]
                wg[l, d, el] = gate[d * half_d:(d + 1) * half_d]
                wu[l, d, el] = up[d * half_d:(d + 1) * half_d]
            return c

        lax.fori_loop(0, E_LOC, one, 0)
        for copy in pairs(l):
            copy.start()
        for part, own, got in stacks:
            emit(part.at[l, dp], own.at[l])

    weight_grads(1, x2)

    def backward_combine(l, phase, ret, grad_y):
        p0[...] = jnp.zeros_like(p0)

        def step(k, carry):
            def one(el, c):
                @pl.when(k > 0)
                def _():
                    giveback(phase, ret, k, el).wait_recv()

                rows = ret[place(k), pl.ds(pl.multiple_of(el * CAP, CAP), CAP)]
                e = partner(k) * E_LOC + el
                p0[...] += dot(onehot(keys[l, 0, pl.ds(e, 1), :]), rows, TN)
                return c

            lax.fori_loop(0, E_LOC, one, 0)
            return carry

        lax.fori_loop(0, EP, step, 0)
        return (grad_y.astype(F32) + p0[...]).astype(BF)

    def grad_input(grad_mixed, m):
        return (grad_mixed.astype(F32) + dot(grad_mixed, m[...], NT)).astype(BF)

    def dense_copies(l):
        copies = []
        for r in range(1, EP * DP):
            peer = (flat + r) % (EP * DP)
            copies.append(pltpu.make_async_remote_copy(
                src_ref=dpart.at[l, peer], dst_ref=dense_out.at[l, r], send_sem=all_send.at[l, r], recv_sem=all_recv.at[l, r],
                device_id={'ep': peer % EP, 'dp': peer // EP}, device_id_type=MESH))
        return copies

    def dense_grad(l, x, grad_mixed):
        part = dot(x, grad_mixed, TN).astype(BF)
        for q in range(EP * DP):
            dpart[l, q] = part[q * 32:(q + 1) * 32]
        for copy in dense_copies(l):
            copy.start()
        emit(dpart.at[l, flat], dense_out.at[l, 0])

    grad_mixed = backward_combine(1, GR_TWO, grt2, dyb[0])
    gmb[0] = grad_input(grad_mixed, vm2)
    spread(GM, gmb)
    dense_grad(1, yb[0], grad_mixed)

    def backward_one(k, carry):
        @pl.when(k == 1)
        def _():
            pass_on(GM, gmb)

        arrive(GM, gmb, k)

        def one(el, c):
            rows = pl.ds(pl.multiple_of(k * CAP, CAP), CAP)
            e = pl.ds(me * E_LOC + el, 1)
            key = keys[0, k, e, :]
            gout[el, rows] = (dot(onehot(key), gmb[k]) * gate_column(key, gates[0, k, e, :])).astype(BF)
            expert_backward(k, el, a1[el, rows], b1[el, rows], vg1, vu1, vw1, GR_ONE, grt1)
            return c

        lax.fori_loop(0, E_LOC, one, 0)
        return carry

    lax.fori_loop(0, EP, backward_one, 0)
    weight_grads(0, x1)
    grad_mixed = backward_combine(0, GR_ONE, grt1, gmb[0])
    dense_grad(0, xin[0], grad_mixed)
    dxb[...] = grad_input(grad_mixed, vm1)
    emit(dxb, dx_out)

    for k in range(1, EP):
        tell(k).wait_send()
        for phase, buf in ((O_ONE, oret), (GR_TWO, grt2), (GR_ONE, grt1)):
            for el in range(E_LOC):
                giveback(phase, buf, k, el).wait_send()
    for phase, buf in ((X_IN, xin), (DY, dyb), (Y_ONE, yb), (GM, gmb)):
        for k in (1, 2):
            for piece in range(2):
                ship(phase, buf, k, piece).wait_send()
            relay(phase, buf, k).wait_send()
    for l in range(2):
        for copy in pairs(l) + dense_copies(l):
            copy.wait()
    for copy in outs:
        copy.wait()


def finish(dx, own_g, own_u, own_w, got_g, got_u, got_w, dense,
           dx_out, gd1, gg1, gu1, gw1, gd2, gg2, gu2, gw2,
           vx, vog, vou, vow, vrg, vru, vrw, vd, vsum, in_sem, out_sem):
    loads = []

    def load(src, dst):
        copy = pltpu.make_async_copy(src, dst, in_sem.at[len(loads)])
        copy.start()
        loads.append(copy)
        return copy

    dense_in = load(dense, vd)
    dx_in = load(dx, vx)
    stacks = []
    for l, outs in enumerate(((gg1, gu1, gw1), (gg2, gu2, gw2))):
        for own, got, vo, vr, out in zip((own_g, own_u, own_w), (got_g, got_u, got_w), (vog, vou, vow), (vrg, vru, vrw), outs):
            stacks.append((load(own.at[l], vo.at[l]), load(got.at[l], vr.at[l]), vo.at[l], vr.at[l], out))
    stores = []

    def store(src, dst):
        copy = pltpu.make_async_copy(src, dst, out_sem.at[len(stores)])
        copy.start()
        stores.append(copy)

    dense_in.wait()
    for l, out in enumerate((gd1, gd2)):
        vsum[l] = jnp.sum(vd[l].astype(F32), axis=0).astype(BF)
        store(vsum.at[l], out)
    dx_in.wait()
    store(vx, dx_out)
    for first, second, vo, vr, out in stacks:
        first.wait()
        second.wait()
        vo[...] = (vo[...].astype(F32) + vr[...].astype(F32)).astype(BF)
        store(vo, out)
    for copy in stores:
        copy.wait()


def solution(mesh):
    tok_spec = P(('dp', 'ep'), None)
    exp_spec = P('ep', None, None)
    layer_specs = (P(None, None), tok_spec, tok_spec, exp_spec, exp_spec, exp_spec)
    grad_specs = (P(('dp', 'ep'), None), P('ep', 'dp', None), P('ep', 'dp', None), P('ep', None, 'dp'))

    def local_step(tokens, dy_out, dense_w1, route_idx1, route_gate1, w_gate1, w_up1, w_down1, dense_w2, route_idx2, route_gate2, w_gate2, w_up2, w_down2):
        hbm = pl.BlockSpec(memory_space=pl.ANY)
        half = D // DP

        def sds(*shape):
            return jax.ShapeDtypeStruct(shape, BF)

        grads = (sds(32, D), sds(E_LOC, half, FF), sds(E_LOC, half, FF), sds(E_LOC, FF, half))
        stacks = (sds(2, E_LOC, half, FF), sds(2, E_LOC, half, FF), sds(2, E_LOC, FF, half))
        vm = pltpu.VMEM
        dma = pltpu.SemaphoreType.DMA
        weights = [vm((D, D), BF), vm((E_LOC, D, FF), BF), vm((E_LOC, D, FF), BF), vm((E_LOC, FF, D), BF)]
        spread_buf = vm((EP, TOK, D), BF)
        ret_buf = vm((2 * EP - 1, TOK, D), BF)
        scratch = [vm((2, 2, TOK), jnp.int32), vm((2, 2, TOK), F32)]
        scratch += [vm((EP, 8, TOK), F32), spread_buf, spread_buf, spread_buf, spread_buf, ret_buf, ret_buf, ret_buf]
        scratch += weights + weights
        scratch += [vm((TOK, TOK), BF), vm((2, EP, 8, TOK), jnp.int32), vm((2, EP, 8, TOK), F32), vm((2, 8, TOK), jnp.int32)]
        scratch += [vm((E_LOC, EP * CAP, D), BF)] * 3
        scratch += [vm((E_LOC, EP * CAP, FF), F32)] * 2
        scratch += [vm((E_LOC, EP * CAP, FF), BF)] * 3
        scratch += [vm((TOK, D), BF), vm((TOK, D), F32), vm((TOK, D), F32)]
        scratch += [vm((2, DP, E_LOC, half, FF), BF)] * 2 + [vm((2, DP, E_LOC, FF, half), BF)]
        scratch += [vm((2, EP * DP, 32, D), BF), vm((TOK, D), BF)]
        scratch += [dma((14,)), dma((EP,)), dma((EP,)), dma((4, EP, 2)), dma((4, EP, 2)), dma((3, EP, 2)), dma((3, EP, 2)),
                    dma((2, 3)), dma((2, 3)), dma((2, 8)), dma((2, 8)), dma((9,))]
        parts = pl.pallas_call(
            kernel,
            out_shape=(sds(TOK, D),) + stacks + stacks + (sds(2, EP * DP, 32, D),),
            in_specs=[hbm] * 14,
            out_specs=(hbm,) * 8,
            scratch_shapes=scratch,
            name='moe_backward',
            compiler_params=pltpu.CompilerParams(collective_id=0, has_side_effects=True, vmem_limit_bytes=67043328),
        )(tokens, dy_out, route_idx1.T, route_idx2.T, route_gate1.T, route_gate2.T,
          dense_w1, w_gate1, w_up1, w_down1, dense_w2, w_gate2, w_up2, w_down2)
        return pl.pallas_call(
            finish,
            out_shape=(sds(TOK, D),) + grads + grads,
            in_specs=[hbm] * 8,
            out_specs=(hbm,) * 9,
            scratch_shapes=[vm(p.shape, BF) for p in parts] + [vm((2, 32, D), BF), dma((14,)), dma((9,))],
            name='finish',
        )(*parts)

    return jax.shard_map(local_step, mesh=mesh, in_specs=(tok_spec, tok_spec) + layer_specs + layer_specs,
                         out_specs=(tok_spec,) + grad_specs + grad_specs, check_vma=False)
```

```python
import jax
import jax.numpy as jnp
from jax import lax
from jax.experimental import pallas as pl
from jax.experimental.pallas import tpu as pltpu
from jax.sharding import PartitionSpec as P

MESH = pl.DeviceIdType.MESH
BF = jnp.bfloat16
F32 = jnp.float32
NN = ((1,), (0,))
NT = ((1,), (1,))
TN = ((0,), (0,))
EP = 4
DP = 2
E_LOC = 2
TOK = 512
CAP = 256
D = 256
FF = 896
LANES = 128
TILES = FF // LANES
VMEM_LIMIT = 54 * 1024 * 1024
X_IN, DY, Y_ONE, GM = range(4)
O_ONE, GR_TWO, GR_ONE = range(3)


def dot(a, b, dims=NN):
    return lax.dot_general(a, b, (dims, ((), ())), preferred_element_type=F32)


def place(k):
    return k + 3 * ((k + 3) // 4)


def unit(i):
    q = i // 2
    mid = (q + 1) // 2 % 2
    return mid * (1 + i % 2) + (1 - mid) * q, mid * (q - 1) + (1 - mid) * (i % 2)


def onehot(key_row):
    rows = lax.broadcasted_iota(jnp.int32, (CAP, TOK), 0)
    return jnp.where(rows == key_row, 1.0, 0.0).astype(BF)


def gate_column(key_row, gate_row):
    rows = lax.broadcasted_iota(jnp.int32, (CAP, TOK), 0)
    return jnp.sum(jnp.where(rows == key_row, gate_row, 0.0), axis=1, keepdims=True)


def kernel(tokens, dy, idx1, idx2, gate1, gate2, m1, g1, u1, w1, m2, g2, u2, w2,
           dx_out, wg, wu, wd, got_g, got_u, got_w, dpart, dense_got,
           ibuf, gbuf, rt, xin, dyb, yb, gmb, oret, grt2, grt1,
           vm1, vgu1, vw1, vm2, vgu2, vw2,
           tri, keys, gates, keyj, picks, x1, x2, gout, ab1, hb, gab, ub, p0, p1,
           loc_sem, rt_send, rt_recv, ag_send, ag_recv, ret_send, ret_recv, dp_send, dp_recv, all_send, all_recv):
    me = lax.axis_index('ep')
    dp = lax.axis_index('dp')
    flat = dp * EP + me
    other = 1 - dp

    barrier = pltpu.get_barrier_semaphore()
    for r in range(1, EP * DP):
        peer = (flat + r) % (EP * DP)
        pl.semaphore_signal(barrier, inc=1, device_id={'ep': peer % EP, 'dp': peer // EP}, device_id_type=MESH)

    def partner(k):
        return (me // 2 + k // 2) % 2 * 2 + (me + k) % 2

    def weight_loads(m, g, u, w, vm, vgu, vw):
        pieces = [(m, vm), (w, vw)]
        for n in range(TILES):
            cols = pl.ds(n * LANES, LANES)
            pieces += [(g.at[:, :, cols], vgu.at[:, n, :, pl.ds(0, LANES)]), (u.at[:, :, cols], vgu.at[:, n, :, pl.ds(LANES, LANES)])]
        return pieces

    loads = [(idx1, ibuf.at[0]), (idx2, ibuf.at[1]), (gate1, gbuf.at[0]), (gate2, gbuf.at[1]), (tokens, xin.at[0]), (dy, dyb.at[0])]
    loads += weight_loads(m1, g1, u1, w1, vm1, vgu1, vw1)
    loads_one = len(loads)
    loads += weight_loads(m2, g2, u2, w2, vm2, vgu2, vw2)
    loads = [pltpu.make_async_copy(src, dst, loc_sem.at[n]) for n, (src, dst) in enumerate(loads)]
    for copy in loads:
        copy.start()

    for copy in loads[:4]:
        copy.wait()
    rt[0] = jnp.concatenate([ibuf[0].astype(F32), ibuf[1].astype(F32), gbuf[0], gbuf[1]], axis=0)
    loads[4].wait()
    pl.semaphore_wait(barrier, EP * DP - 1)

    def remote(src, dst, send, recv, k):
        return pltpu.make_async_remote_copy(src_ref=src, dst_ref=dst, send_sem=send, recv_sem=recv,
                                            device_id={'ep': partner(k)}, device_id_type=MESH)

    def tell(k):
        return remote(rt.at[0], rt.at[k], rt_send.at[k], rt_recv.at[k], k)

    def half(h):
        return pl.ds(h * CAP, CAP)

    def ship(phase, buf, k, piece):
        rows = half(piece if k == 1 else 1 - piece)
        return remote(buf.at[0, rows], buf.at[k, rows], ag_send.at[phase, k, piece], ag_recv.at[phase, k, piece], k)

    def relay(phase, buf, via):
        rows = half(via - 1)
        return remote(buf.at[via, rows], buf.at[3, rows], ag_send.at[phase, 3, via - 1], ag_recv.at[phase, 3, via - 1], 3 - via)

    def spread(phase, buf):
        for piece in range(2):
            for k in (1, 2):
                ship(phase, buf, k, piece).start()

    def pass_on(phase, buf):
        for via in (1, 2):
            ship(phase, buf, via, 0).wait_recv()
            relay(phase, buf, via).start()

    def arrive(phase, buf, k):
        for near in (1, 2):
            @pl.when(k == near)
            def _():
                ship(phase, buf, near, 1).wait_recv()

        @pl.when(k == 3)
        def _():
            for via in (1, 2):
                relay(phase, buf, via).wait_recv()

    def giveback(phase, buf, k, el):
        rows = pl.ds(pl.multiple_of(el * CAP, CAP), CAP)
        return remote(buf.at[k, rows], buf.at[k + 3, rows], ret_send.at[phase, k, el], ret_recv.at[phase, k, el], k)

    for k in range(1, EP):
        tell(k).start()

    @pl.when(dp == 1)
    def _():
        loads[5].wait()
        spread(DY, dyb)

    spread(X_IN, xin)

    tri[...] = jnp.where(lax.broadcasted_iota(jnp.int32, (TOK, TOK), 0) < lax.broadcasted_iota(jnp.int32, (TOK, TOK), 1), 1.0, 0.0).astype(BF)
    expert = lax.broadcasted_iota(jnp.int32, (E_LOC * EP, TOK), 0).astype(F32)

    def make_keys(k):
        info = rt[k]
        for l in range(2):
            hit0 = info[2 * l:2 * l + 1] == expert
            hit1 = info[2 * l + 1:2 * l + 2] == expert
            both = jnp.where(hit0, 1.0, jnp.where(hit1, 1.0, 0.0))
            rank = dot(both.astype(BF), tri[...]).astype(jnp.int32)
            keys[l, k] = jnp.where(both > 0.5, rank, -1)
            gates[l, k] = jnp.where(hit0, info[4 + 2 * l:5 + 2 * l], jnp.where(hit1, info[5 + 2 * l:6 + 2 * l], 0.0))
        return info

    info = make_keys(0)
    for j in range(2):
        keyj[j] = jnp.where(info[j:j + 1] == expert, keys[0, 0], -1)
    for copy in loads[6:loads_one]:
        copy.wait()

    def build_picks(*sources):
        slots = lax.broadcasted_iota(jnp.int32, (TOK, CAP), 1)
        for j, source in enumerate(sources):
            rows = [source[pl.ds(partner(k) * E_LOC + el, 1), :] for k in range(EP) for el in range(E_LOC)]
            cols = jnp.transpose(jnp.concatenate(rows, axis=0))
            for r in range(EP * E_LOC):
                picks[j, :, r * CAP:(r + 1) * CAP] = jnp.where(slots == cols[:, r:r + 1], 1.0, 0.0).astype(BF)

    def picked(j, ret, last):
        if last:
            return dot(picks[j, :, 3 * TOK:], ret[6])
        return dot(picks[j, :, :TOK], ret[0]) + dot(picks[j, :, TOK:3 * TOK], ret[4:6].reshape(2 * TOK, D))

    def silu_parts(a):
        sig = 0.5 * jnp.tanh(0.5 * a) + 0.5
        return sig, a * sig

    def groups():
        return [range(n, min(n + 2, TILES)) for n in range(0, TILES, 2)]

    def mixed(x, m):
        return (x.astype(F32) + dot(x, m[...])).astype(BF)

    def forward_one(i, carry):
        k, el = unit(i)

        @pl.when(i == 2)
        def _():
            build_picks(keyj.at[0], keyj.at[1])

            @pl.when(dp == 1)
            def _():
                pass_on(DY, dyb)

            pass_on(X_IN, xin)

        @pl.when(el == 0)
        def _():
            @pl.when(k > 0)
            def _():
                tell(k).wait_recv()
                make_keys(k)

            arrive(X_IN, xin, k)
            ub[k] = mixed(xin[k], vm1)

        rows = pl.ds(pl.multiple_of(k * CAP, CAP), CAP)
        key = keys[0, k, pl.ds(me * E_LOC + el, 1), :]
        x = dot(onehot(key), ub[k]).astype(BF)
        x1[el, rows] = x
        out = jnp.zeros((CAP, D), F32)
        for group in groups():
            h = []
            for n in group:
                ab = dot(x, vgu1[el, n])
                ab1[el, n, rows] = ab
                h.append((silu_parts(ab[:, :LANES])[1] * ab[:, LANES:]).astype(BF))
            out += dot(jnp.concatenate(h, axis=1), vw1[el, group[0] * LANES:(group[-1] + 1) * LANES])
        oret[k, pl.ds(pl.multiple_of(el * CAP, CAP), CAP)] = out.astype(BF)

        @pl.when(k > 0)
        def _():
            giveback(O_ONE, oret, k, el).start()
        return carry

    lax.fori_loop(0, EP * E_LOC, forward_one, 0)

    @pl.when(dp == 0)
    def _():
        loads[5].wait()
        spread(DY, dyb)

    for copy in loads[loads_one:]:
        copy.wait()

    def collect(phase, ret, ks):
        for k in ks:
            for el in range(E_LOC):
                giveback(phase, ret, k, el).wait_recv()

    collect(O_ONE, oret, (1, 2))
    p0[...] = picked(0, oret, False)
    p1[...] = picked(1, oret, False)
    gcol0 = jnp.transpose(jnp.broadcast_to(rt[0, 4:5], (8, TOK)))[:, :1]
    gcol1 = jnp.transpose(jnp.broadcast_to(rt[0, 5:6], (8, TOK)))[:, :1]
    collect(O_ONE, oret, (3,))
    out0 = p0[...] + picked(0, oret, True)
    out1 = p1[...] + picked(1, oret, True)
    yb[0] = (ub[0].astype(F32) + (gcol0 * out0 + gcol1 * out1)).astype(BF)
    spread(Y_ONE, yb)

    def expert_backward(k, el, first, vgu, vw, phase, ret):
        rows = pl.ds(pl.multiple_of(k * CAP, CAP), CAP)
        go = gout[el, rows]
        back = jnp.zeros((CAP, D), F32)
        for group in groups():
            cols = slice(group[0] * LANES, (group[-1] + 1) * LANES)
            grad_h = dot(go, vw[el, cols], NT).astype(BF).astype(F32)
            for n in group:
                ab = first(n)
                a, b = ab[:, :LANES], ab[:, LANES:]
                dh = grad_h[:, (n - group[0]) * LANES:(n - group[0] + 1) * LANES]
                sig, s = silu_parts(a)
                hb[el, rows, n * LANES:(n + 1) * LANES] = (s * b).astype(BF)
                grad_a = (dh * b * (sig + s * (1.0 - sig))).astype(BF)
                grad_b = (dh * s).astype(BF)
                grads = jnp.concatenate([grad_a, grad_b], axis=1)
                gab[el, n, rows] = grads
                back += dot(grads, vgu[el, n], NT)
        ret[k, pl.ds(pl.multiple_of(el * CAP, CAP), CAP)] = back.astype(BF)

        @pl.when(k > 0)
        def _():
            giveback(phase, ret, k, el).start()

    def layer_two(i, carry):
        k, el = unit(i)

        @pl.when(i == 2)
        def _():
            build_picks(keys.at[1, 0])

            @pl.when(dp == 0)
            def _():
                pass_on(DY, dyb)

            pass_on(Y_ONE, yb)

        @pl.when(el == 0)
        def _():
            arrive(DY, dyb, k)
            arrive(Y_ONE, yb, k)
            ub[k] = mixed(yb[k], vm2)

        rows = pl.ds(pl.multiple_of(k * CAP, CAP), CAP)
        e = pl.ds(me * E_LOC + el, 1)
        key = keys[1, k, e, :]
        pick = onehot(key)
        x = dot(pick, ub[k]).astype(BF)
        x2[el, rows] = x
        gout[el, rows] = (dot(pick, dyb[k]) * gate_column(key, gates[1, k, e, :])).astype(BF)
        expert_backward(k, el, lambda n: dot(x, vgu2[el, n]), vgu2, vw2, GR_TWO, grt2)
        return carry

    lax.fori_loop(0, EP * E_LOC, layer_two, 0)

    stacks = ((wg, got_g), (wu, got_u), (wd, got_w))

    def pairs(l):
        return [pltpu.make_async_remote_copy(src_ref=part.at[l, other], dst_ref=got.at[l], send_sem=dp_send.at[l, n],
                                             recv_sem=dp_recv.at[l, n], device_id={'dp': other}, device_id_type=MESH)
                for n, (part, got) in enumerate(stacks)]

    def weight_grads(l, x_all, el):
        half_d = D // DP
        x = x_all[el]
        down = dot(hb[el], gout[el], TN).astype(BF)
        for d in range(DP):
            wd[l, d, el] = down[:, d * half_d:(d + 1) * half_d]

        for n in range(TILES):
            cols = slice(n * LANES, (n + 1) * LANES)
            both = dot(x, gab[el, n], TN).astype(BF)
            for d in range(DP):
                rows = slice(d * half_d, (d + 1) * half_d)
                wg[l, d, el, :, cols] = both[rows, :LANES]
                wu[l, d, el, :, cols] = both[rows, LANES:]

    def send_weight_grads(l):
        for copy in pairs(l):
            copy.start()

    weight_grads(1, x2, 0)

    def backward_combine(phase, ret, grad_y):
        collect(phase, ret, (1, 2))
        p0[...] = picked(0, ret, False)
        collect(phase, ret, (3,))
        return (grad_y.astype(F32) + (p0[...] + picked(0, ret, True))).astype(BF)

    def grad_input(grad_mixed, m):
        return (grad_mixed.astype(F32) + dot(grad_mixed, m[...], NT)).astype(BF)

    def dense_copies(l):
        copies = []
        for r in range(1, EP * DP):
            peer = (flat + r) % (EP * DP)
            copies.append(pltpu.make_async_remote_copy(
                src_ref=dpart.at[l, peer], dst_ref=dense_got.at[l, r], send_sem=all_send.at[l, r], recv_sem=all_recv.at[l, r],
                device_id={'ep': peer % EP, 'dp': peer // EP}, device_id_type=MESH))
        return copies

    def dense_grad(l, x, grad_mixed):
        part = dot(x, grad_mixed, TN).astype(BF)
        for q in range(EP * DP):
            dpart[l, q] = part[q * 32:(q + 1) * 32]
        for copy in dense_copies(l):
            copy.start()

    grad_mixed = backward_combine(GR_TWO, grt2, dyb[0])
    gmb[0] = grad_input(grad_mixed, vm2)
    spread(GM, gmb)
    weight_grads(1, x2, 1)
    send_weight_grads(1)
    dense_grad(1, yb[0], grad_mixed)

    def backward_one(i, carry):
        k, el = unit(i)

        @pl.when(i == 2)
        def _():
            build_picks(keys.at[0, 0])

        @pl.when(i == 0)
        def _():
            pass_on(GM, gmb)

        @pl.when(el == 0)
        def _():
            arrive(GM, gmb, k)

        rows = pl.ds(pl.multiple_of(k * CAP, CAP), CAP)
        e = pl.ds(me * E_LOC + el, 1)
        key = keys[0, k, e, :]
        gout[el, rows] = (dot(onehot(key), gmb[k]) * gate_column(key, gates[0, k, e, :])).astype(BF)
        expert_backward(k, el, lambda n: ab1[el, n, rows], vgu1, vw1, GR_ONE, grt1)
        return carry

    lax.fori_loop(0, EP * E_LOC, backward_one, 0)
    weight_grads(0, x1, 0)
    weight_grads(0, x1, 1)
    send_weight_grads(0)
    grad_mixed = backward_combine(GR_ONE, grt1, gmb[0])
    dense_grad(0, xin[0], grad_mixed)
    dx_out[...] = grad_input(grad_mixed, vm1)

    for k in range(1, EP):
        tell(k).wait_send()
        for phase, buf in ((O_ONE, oret), (GR_TWO, grt2), (GR_ONE, grt1)):
            for el in range(E_LOC):
                giveback(phase, buf, k, el).wait_send()
    for phase, buf in ((X_IN, xin), (DY, dyb), (Y_ONE, yb), (GM, gmb)):
        for k in (1, 2):
            for piece in range(2):
                ship(phase, buf, k, piece).wait_send()
            relay(phase, buf, k).wait_send()
    for l in range(2):
        for copy in pairs(l) + dense_copies(l):
            copy.wait()


def finish(dx, wg, wu, wd, got_g, got_u, got_w, dpart, dense_got,
           dx_out, gd1, gg1, gu1, gw1, gd2, gg2, gu2, gw2,
           vg, vu, vw, vsum, out_sem):
    dp = lax.axis_index('dp')
    flat = dp * EP + lax.axis_index('ep')
    stores = []

    def store(src, dst):
        copy = pltpu.make_async_copy(src, dst, out_sem.at[len(stores)])
        copy.start()
        stores.append(copy)

    store(dx, dx_out)
    for l, outs in enumerate(((gg1, gu1, gw1), (gg2, gu2, gw2))):
        for own, got, total, out in zip((wg, wu, wd), (got_g, got_u, got_w), (vg, vu, vw), outs):
            total[l] = (own[l, dp].astype(F32) + got[l].astype(F32)).astype(BF)
            store(total.at[l], out)
    for l, out in enumerate((gd1, gd2)):
        total = dpart[l, flat].astype(F32)
        for r in range(1, EP * DP):
            total += dense_got[l, r].astype(F32)
        vsum[l] = total.astype(BF)
        store(vsum.at[l], out)
    for copy in stores:
        copy.wait()


def solution(mesh):
    tok_spec = P(('dp', 'ep'), None)
    exp_spec = P('ep', None, None)
    layer_specs = (P(None, None), tok_spec, tok_spec, exp_spec, exp_spec, exp_spec)
    grad_specs = (P(('dp', 'ep'), None), P('ep', 'dp', None), P('ep', 'dp', None), P('ep', None, 'dp'))

    def local_step(tokens, dy_out, dense_w1, route_idx1, route_gate1, w_gate1, w_up1, w_down1, dense_w2, route_idx2, route_gate2, w_gate2, w_up2, w_down2):
        hbm = pl.BlockSpec(memory_space=pl.ANY)
        half = D // DP

        def sds(*shape):
            return jax.ShapeDtypeStruct(shape, BF)

        grads = (sds(32, D), sds(E_LOC, half, FF), sds(E_LOC, half, FF), sds(E_LOC, FF, half))
        vm = pltpu.VMEM
        got = (vm((2, E_LOC, half, FF), BF), vm((2, E_LOC, half, FF), BF), vm((2, E_LOC, FF, half), BF))
        parts = (vm((2, DP, E_LOC, half, FF), BF), vm((2, DP, E_LOC, half, FF), BF), vm((2, DP, E_LOC, FF, half), BF))
        dense = vm((2, EP * DP, 32, D), BF)
        on_chip = pl.BlockSpec(memory_space=pltpu.VMEM)
        dma = pltpu.SemaphoreType.DMA
        weights = [vm((D, D), BF), vm((E_LOC, TILES, D, 2 * LANES), BF), vm((E_LOC, FF, D), BF)]
        spread_buf = vm((EP, TOK, D), BF)
        ret_buf = vm((2 * EP - 1, TOK, D), BF)
        scratch = [vm((2, 2, TOK), jnp.int32), vm((2, 2, TOK), F32)]
        scratch += [vm((EP, 8, TOK), F32), spread_buf, spread_buf, spread_buf, spread_buf, ret_buf, ret_buf, ret_buf]
        scratch += weights + weights
        scratch += [vm((TOK, TOK), BF), vm((2, EP, 8, TOK), jnp.int32), vm((2, EP, 8, TOK), F32), vm((2, 8, TOK), jnp.int32)]
        scratch += [vm((2, TOK, EP * TOK), BF)]
        scratch += [vm((E_LOC, EP * CAP, D), BF)] * 3
        scratch += [vm((E_LOC, TILES, EP * CAP, 2 * LANES), F32), vm((E_LOC, EP * CAP, FF), BF), vm((E_LOC, TILES, EP * CAP, 2 * LANES), BF)]
        scratch += [spread_buf, vm((TOK, D), F32), vm((TOK, D), F32)]
        scratch += [dma((6 + 4 * (TILES + 1),)), dma((EP,)), dma((EP,)), dma((4, EP, 2)), dma((4, EP, 2)), dma((3, EP, 2)), dma((3, EP, 2)),
                    dma((2, 3)), dma((2, 3)), dma((2, 8)), dma((2, 8))]
        results = pl.pallas_call(
            kernel,
            out_shape=(vm((TOK, D), BF),) + parts + got + (dense, dense),
            in_specs=[hbm] * 14,
            out_specs=(on_chip,) * 9,
            scratch_shapes=scratch,
            name='moe_backward',
            compiler_params=pltpu.CompilerParams(collective_id=0, has_side_effects=True, vmem_limit_bytes=VMEM_LIMIT),
        )(tokens, dy_out, route_idx1.T, route_idx2.T, route_gate1.T, route_gate2.T,
          dense_w1, w_gate1, w_up1, w_down1, dense_w2, w_gate2, w_up2, w_down2)
        return pl.pallas_call(
            finish,
            out_shape=(sds(TOK, D),) + grads + grads,
            in_specs=[on_chip] * 9,
            out_specs=(hbm,) * 9,
            scratch_shapes=list(got) + [vm((2, 32, D), BF), dma((9,))],
            name='finish',
            compiler_params=pltpu.CompilerParams(vmem_limit_bytes=16 * 1024 * 1024),
        )(*[pltpu.with_memory_space_constraint(r, pltpu.VMEM) for r in results])

    return jax.shard_map(local_step, mesh=mesh, in_specs=(tok_spec, tok_spec) + layer_specs + layer_specs,
                         out_specs=(tok_spec,) + grad_specs + grad_specs, check_vma=False)
```

```python
import jax
import jax.numpy as jnp
from jax import lax
from jax.experimental import pallas as pl
from jax.experimental.pallas import tpu as pltpu
from jax.sharding import PartitionSpec as P

MESH = pl.DeviceIdType.MESH
BF = jnp.bfloat16
F32 = jnp.float32
NN = ((1,), (0,))
NT = ((1,), (1,))
TN = ((0,), (0,))
EP = 4
DP = 2
E_LOC = 2
TOK = 512
CAP = 256
D = 256
FF = 896
LANES = 128
TILES = FF // LANES
VMEM_LIMIT = 54 * 1024 * 1024
X_IN, DY, Y_ONE, GM = range(4)
O_ONE, GR_TWO, GR_ONE = range(3)


def dot(a, b, dims=NN):
    return lax.dot_general(a, b, (dims, ((), ())), preferred_element_type=F32)


def place(k):
    return k + 3 * ((k + 3) // 4)


def unit(i):
    q = i // 2
    mid = (q + 1) // 2 % 2
    return mid * (1 + i % 2) + (1 - mid) * q, mid * (q - 1) + (1 - mid) * (i % 2)


def onehot(key_row):
    rows = lax.broadcasted_iota(jnp.int32, (CAP, TOK), 0)
    return jnp.where(rows == key_row, 1.0, 0.0).astype(BF)


def gate_column(key_row, gate_row):
    rows = lax.broadcasted_iota(jnp.int32, (CAP, TOK), 0)
    return jnp.sum(jnp.where(rows == key_row, gate_row, 0.0), axis=1, keepdims=True)


def kernel(tokens, dy, idx1, idx2, gate1, gate2, m1, g1, u1, w1, m2, g2, u2, w2,
           dx_out, wg, wu, wd, got_g, got_u, got_w, dpart, dense_got,
           ibuf, gbuf, rt, xin, dyb, yb, gmb, oret, grt2, grt1,
           vm1, vgu1, vw1, vm2, vgu2, vw2,
           tri, keys, gates, keyj, picks, x1, x2, gout, ab1, hb, gab, ub, p0, p1,
           loc_sem, rt_send, rt_recv, ag_send, ag_recv, ret_send, ret_recv, dp_send, dp_recv, all_send, all_recv):
    me = lax.axis_index('ep')
    dp = lax.axis_index('dp')
    flat = dp * EP + me
    other = 1 - dp

    barrier = pltpu.get_barrier_semaphore()
    for r in range(1, EP * DP):
        peer = (flat + r) % (EP * DP)
        pl.semaphore_signal(barrier, inc=1, device_id={'ep': peer % EP, 'dp': peer // EP}, device_id_type=MESH)

    def partner(k):
        return (me // 2 + k // 2) % 2 * 2 + (me + k) % 2

    small = [(idx1, ibuf.at[0]), (idx2, ibuf.at[1]), (gate1, gbuf.at[0]), (gate2, gbuf.at[1]), (tokens, xin.at[0]), (dy, dyb.at[0])]
    small = [pltpu.make_async_copy(src, dst, loc_sem.at[n]) for n, (src, dst) in enumerate(small)]
    for copy in small:
        copy.start()

    def weight_copies(l, m, g, u, w, vm, vgu, vw):
        base = len(small) + 3 * l
        copies = [pltpu.make_async_copy(m, vm, loc_sem.at[base]), pltpu.make_async_copy(w, vw, loc_sem.at[base + 1])]
        for n in range(TILES):
            cols = pl.ds(n * LANES, LANES)
            for src, lanes in ((g, pl.ds(0, LANES)), (u, pl.ds(LANES, LANES))):
                copies.append(pltpu.make_async_copy(src.at[:, :, cols], vgu.at[:, n, :, lanes], loc_sem.at[base + 2]))
        whole = pltpu.make_async_copy(vgu, vgu, loc_sem.at[base + 2])
        return copies, copies[:2] + [whole]

    starts_one, waits_one = weight_copies(0, m1, g1, u1, w1, vm1, vgu1, vw1)
    starts_two, waits_two = weight_copies(1, m2, g2, u2, w2, vm2, vgu2, vw2)
    for copy in starts_one:
        copy.start()

    for copy in small[:4]:
        copy.wait()
    rt[0] = jnp.concatenate([ibuf[0].astype(F32), ibuf[1].astype(F32), gbuf[0], gbuf[1]], axis=0)
    small[4].wait()
    pl.semaphore_wait(barrier, EP * DP - 1)

    def remote(src, dst, send, recv, k):
        return pltpu.make_async_remote_copy(src_ref=src, dst_ref=dst, send_sem=send, recv_sem=recv,
                                            device_id={'ep': partner(k)}, device_id_type=MESH)

    def tell(k):
        return remote(rt.at[0], rt.at[k], rt_send, rt_recv.at[k - 1], k)

    def lane(phase):
        return 1 if phase == DY else 0

    def all_sent(buf, sem):
        remote(buf.at[pl.ds(1, EP - 1)], buf.at[pl.ds(1, EP - 1)], sem, sem, 1).wait_send()

    def half(h):
        return pl.ds(h * CAP, CAP)

    def ship(phase, buf, k, piece):
        rows = half(piece if k == 1 else 1 - piece)
        return remote(buf.at[0, rows], buf.at[k, rows], ag_send.at[lane(phase)], ag_recv.at[lane(phase), k - 1, piece], k)

    def relay(phase, buf, via):
        rows = half(via - 1)
        return remote(buf.at[via, rows], buf.at[3, rows], ag_send.at[lane(phase)], ag_recv.at[lane(phase), 2, via - 1], 3 - via)

    def spread(phase, buf):
        for piece in range(2):
            for k in (1, 2):
                ship(phase, buf, k, piece).start()

    def pass_on(phase, buf):
        for via in (1, 2):
            ship(phase, buf, via, 0).wait_recv()
            relay(phase, buf, via).start()

    def arrive(phase, buf, k):
        for near in (1, 2):
            @pl.when(k == near)
            def _():
                ship(phase, buf, near, 1).wait_recv()

        @pl.when(k == 3)
        def _():
            for via in (1, 2):
                relay(phase, buf, via).wait_recv()

    def giveback(phase, buf, k, el):
        rows = pl.ds(pl.multiple_of(el * CAP, CAP), CAP)
        return remote(buf.at[k, rows], buf.at[k + 3, rows], ret_send, ret_recv.at[k - 1, el], k)

    for k in range(1, EP):
        tell(k).start()

    @pl.when(dp == 1)
    def _():
        small[5].wait()
        spread(DY, dyb)

    spread(X_IN, xin)
    for copy in starts_two:
        copy.start()

    tri[...] = jnp.where(lax.broadcasted_iota(jnp.int32, (TOK, TOK), 0) < lax.broadcasted_iota(jnp.int32, (TOK, TOK), 1), 1.0, 0.0).astype(BF)
    expert = lax.broadcasted_iota(jnp.int32, (E_LOC * EP, TOK), 0).astype(F32)

    def make_keys(k):
        info = rt[k]
        for l in range(2):
            hit0 = info[2 * l:2 * l + 1] == expert
            hit1 = info[2 * l + 1:2 * l + 2] == expert
            both = jnp.where(hit0, 1.0, jnp.where(hit1, 1.0, 0.0))
            rank = dot(both.astype(BF), tri[...]).astype(jnp.int32)
            keys[l, k] = jnp.where(both > 0.5, rank, -1)
            gates[l, k] = jnp.where(hit0, info[4 + 2 * l:5 + 2 * l], jnp.where(hit1, info[5 + 2 * l:6 + 2 * l], 0.0))
        return info

    info = make_keys(0)
    for j in range(2):
        keyj[j] = jnp.where(info[j:j + 1] == expert, keys[0, 0], -1)
    for copy in waits_one:
        copy.wait()

    def build_picks(*sources):
        slots = lax.broadcasted_iota(jnp.int32, (TOK, CAP), 1)
        for j, source in enumerate(sources):
            rows = [source[pl.ds(partner(k) * E_LOC + el, 1), :] for k in range(EP) for el in range(E_LOC)]
            cols = jnp.transpose(jnp.concatenate(rows, axis=0))
            for r in range(EP * E_LOC):
                picks[j, :, r * CAP:(r + 1) * CAP] = jnp.where(slots == cols[:, r:r + 1], 1.0, 0.0).astype(BF)

    def picked(j, ret, last):
        if last:
            return dot(picks[j, :, 3 * TOK:], ret[6])
        return dot(picks[j, :, :TOK], ret[0]) + dot(picks[j, :, TOK:3 * TOK], ret[4:6].reshape(2 * TOK, D))

    def silu_parts(a):
        sig = 0.5 * jnp.tanh(0.5 * a) + 0.5
        return sig, a * sig

    def groups():
        return [range(n, min(n + 2, TILES)) for n in range(0, TILES, 2)]

    def mixed(x, m):
        return (x.astype(F32) + dot(x, m[...])).astype(BF)

    def forward_one(i, carry):
        k, el = unit(i)

        @pl.when(i == 2)
        def _():
            build_picks(keyj.at[0], keyj.at[1])

            @pl.when(dp == 1)
            def _():
                pass_on(DY, dyb)

            pass_on(X_IN, xin)

        @pl.when(el == 0)
        def _():
            @pl.when(k > 0)
            def _():
                tell(k).wait_recv()
                make_keys(k)

            arrive(X_IN, xin, k)
            ub[k] = mixed(xin[k], vm1)

        rows = pl.ds(pl.multiple_of(k * CAP, CAP), CAP)
        key = keys[0, k, pl.ds(me * E_LOC + el, 1), :]
        x = dot(onehot(key), ub[k]).astype(BF)
        x1[el, rows] = x
        out = jnp.zeros((CAP, D), F32)
        for group in groups():
            h = []
            for n in group:
                ab = dot(x, vgu1[el, n])
                ab1[el, n, rows] = ab
                h.append((silu_parts(ab[:, :LANES])[1] * ab[:, LANES:]).astype(BF))
            out += dot(jnp.concatenate(h, axis=1), vw1[el, group[0] * LANES:(group[-1] + 1) * LANES])
        oret[k, pl.ds(pl.multiple_of(el * CAP, CAP), CAP)] = out.astype(BF)

        @pl.when(k > 0)
        def _():
            giveback(O_ONE, oret, k, el).start()
        return carry

    lax.fori_loop(0, EP * E_LOC, forward_one, 0)

    @pl.when(dp == 0)
    def _():
        small[5].wait()
        spread(DY, dyb)

    for copy in waits_two:
        copy.wait()

    def collect(phase, ret, ks):
        for k in ks:
            for el in range(E_LOC):
                giveback(phase, ret, k, el).wait_recv()

    collect(O_ONE, oret, (1, 2))
    p0[...] = picked(0, oret, False)
    p1[...] = picked(1, oret, False)
    gcol0 = jnp.transpose(jnp.broadcast_to(rt[0, 4:5], (8, TOK)))[:, :1]
    gcol1 = jnp.transpose(jnp.broadcast_to(rt[0, 5:6], (8, TOK)))[:, :1]
    collect(O_ONE, oret, (3,))
    out0 = p0[...] + picked(0, oret, True)
    out1 = p1[...] + picked(1, oret, True)
    yb[0] = (ub[0].astype(F32) + (gcol0 * out0 + gcol1 * out1)).astype(BF)
    all_sent(xin, ag_send.at[0])
    spread(Y_ONE, yb)

    def expert_backward(k, el, first, vgu, vw, phase, ret):
        rows = pl.ds(pl.multiple_of(k * CAP, CAP), CAP)
        go = gout[el, rows]
        back = jnp.zeros((CAP, D), F32)
        for group in groups():
            cols = slice(group[0] * LANES, (group[-1] + 1) * LANES)
            grad_h = dot(go, vw[el, cols], NT).astype(BF).astype(F32)
            for n in group:
                ab = first(n)
                a, b = ab[:, :LANES], ab[:, LANES:]
                dh = grad_h[:, (n - group[0]) * LANES:(n - group[0] + 1) * LANES]
                sig, s = silu_parts(a)
                hb[el, rows, n * LANES:(n + 1) * LANES] = (s * b).astype(BF)
                grad_a = (dh * b * (sig + s * (1.0 - sig))).astype(BF)
                grad_b = (dh * s).astype(BF)
                grads = jnp.concatenate([grad_a, grad_b], axis=1)
                gab[el, n, rows] = grads
                back += dot(grads, vgu[el, n], NT)
        ret[k, pl.ds(pl.multiple_of(el * CAP, CAP), CAP)] = back.astype(BF)

        @pl.when(k > 0)
        def _():
            giveback(phase, ret, k, el).start()

    all_sent(oret, ret_send)

    def layer_two(i, carry):
        k, el = unit(i)

        @pl.when(i == 2)
        def _():
            build_picks(keys.at[1, 0])

            @pl.when(dp == 0)
            def _():
                pass_on(DY, dyb)

            pass_on(Y_ONE, yb)

        @pl.when(el == 0)
        def _():
            arrive(DY, dyb, k)
            arrive(Y_ONE, yb, k)
            ub[k] = mixed(yb[k], vm2)

        rows = pl.ds(pl.multiple_of(k * CAP, CAP), CAP)
        e = pl.ds(me * E_LOC + el, 1)
        key = keys[1, k, e, :]
        pick = onehot(key)
        x = dot(pick, ub[k]).astype(BF)
        x2[el, rows] = x
        gout[el, rows] = (dot(pick, dyb[k]) * gate_column(key, gates[1, k, e, :])).astype(BF)
        expert_backward(k, el, lambda n: dot(x, vgu2[el, n]), vgu2, vw2, GR_TWO, grt2)
        return carry

    lax.fori_loop(0, EP * E_LOC, layer_two, 0)

    stacks = ((wg, got_g), (wu, got_u), (wd, got_w))

    def pairs(l):
        return [pltpu.make_async_remote_copy(src_ref=part.at[l, other], dst_ref=got.at[l], send_sem=dp_send.at[n],
                                             recv_sem=dp_recv.at[l, n], device_id={'dp': other}, device_id_type=MESH)
                for n, (part, got) in enumerate(stacks)]

    def weight_grads(l, x_all, el):
        half_d = D // DP
        x = x_all[el]
        down = dot(hb[el], gout[el], TN).astype(BF)
        for d in range(DP):
            wd[l, d, el] = down[:, d * half_d:(d + 1) * half_d]

        for n in range(TILES):
            cols = slice(n * LANES, (n + 1) * LANES)
            both = dot(x, gab[el, n], TN).astype(BF)
            for d in range(DP):
                rows = slice(d * half_d, (d + 1) * half_d)
                wg[l, d, el, :, cols] = both[rows, :LANES]
                wu[l, d, el, :, cols] = both[rows, LANES:]

    def send_weight_grads(l):
        if l == 0:
            for copy in pairs(1):
                copy.wait_send()
        for copy in pairs(l):
            copy.start()

    weight_grads(1, x2, 0)

    def backward_combine(phase, ret, grad_y):
        collect(phase, ret, (1, 2))
        p0[...] = picked(0, ret, False)
        collect(phase, ret, (3,))
        return (grad_y.astype(F32) + (p0[...] + picked(0, ret, True))).astype(BF)

    def grad_input(grad_mixed, m):
        return (grad_mixed.astype(F32) + dot(grad_mixed, m[...], NT)).astype(BF)

    def dense_copies(l):
        copies = []
        for r in range(1, EP * DP):
            peer = (flat + r) % (EP * DP)
            copies.append(pltpu.make_async_remote_copy(
                src_ref=dpart.at[l, peer], dst_ref=dense_got.at[l, r], send_sem=all_send.at[l], recv_sem=all_recv.at[l],
                device_id={'ep': peer % EP, 'dp': peer // EP}, device_id_type=MESH))
        return copies

    def dense_grad(l, x, grad_mixed):
        part = dot(x, grad_mixed, TN).astype(BF)
        for q in range(EP * DP):
            dpart[l, q] = part[q * 32:(q + 1) * 32]
        for copy in dense_copies(l):
            copy.start()

    grad_mixed = backward_combine(GR_TWO, grt2, dyb[0])
    gmb[0] = grad_input(grad_mixed, vm2)
    all_sent(yb, ag_send.at[0])
    spread(GM, gmb)
    weight_grads(1, x2, 1)
    send_weight_grads(1)
    dense_grad(1, yb[0], grad_mixed)

    all_sent(grt2, ret_send)

    def backward_one(i, carry):
        k, el = unit(i)

        @pl.when(i == 2)
        def _():
            build_picks(keys.at[0, 0])

        @pl.when(i == 1)
        def _():
            pass_on(GM, gmb)

        @pl.when(el == 0)
        def _():
            arrive(GM, gmb, k)

        rows = pl.ds(pl.multiple_of(k * CAP, CAP), CAP)
        e = pl.ds(me * E_LOC + el, 1)
        key = keys[0, k, e, :]
        gout[el, rows] = (dot(onehot(key), gmb[k]) * gate_column(key, gates[0, k, e, :])).astype(BF)
        expert_backward(k, el, lambda n: ab1[el, n, rows], vgu1, vw1, GR_ONE, grt1)
        return carry

    lax.fori_loop(0, EP * E_LOC, backward_one, 0)
    weight_grads(0, x1, 0)
    weight_grads(0, x1, 1)
    send_weight_grads(0)
    grad_mixed = backward_combine(GR_ONE, grt1, gmb[0])
    dense_grad(0, xin[0], grad_mixed)
    dx_out[...] = grad_input(grad_mixed, vm1)

    all_sent(rt, rt_send)
    all_sent(dyb, ag_send.at[1])
    all_sent(gmb, ag_send.at[0])
    all_sent(grt1, ret_send)
    for copy in pairs(1):
        copy.wait_recv()
    for copy in pairs(0):
        copy.wait()
    for l in range(2):
        whole = pl.ds(1, EP * DP - 1)
        pltpu.make_async_remote_copy(src_ref=dpart.at[l, whole], dst_ref=dense_got.at[l, whole], send_sem=all_send.at[l], recv_sem=all_recv.at[l],
                                     device_id={'dp': other}, device_id_type=MESH).wait()


def finish(dx, wg, wu, wd, got_g, got_u, got_w, dpart, dense_got,
           dx_out, gd1, gg1, gu1, gw1, gd2, gg2, gu2, gw2,
           vg, vu, vw, vsum, out_sem):
    dp = lax.axis_index('dp')
    flat = dp * EP + lax.axis_index('ep')
    stores = []

    def store(src, dst):
        copy = pltpu.make_async_copy(src, dst, out_sem.at[len(stores)])
        copy.start()
        stores.append(copy)

    store(dx, dx_out)
    for l, outs in enumerate(((gg1, gu1, gw1), (gg2, gu2, gw2))):
        for own, got, total, out in zip((wg, wu, wd), (got_g, got_u, got_w), (vg, vu, vw), outs):
            total[l] = (own[l, dp].astype(F32) + got[l].astype(F32)).astype(BF)
            store(total.at[l], out)
    for l, out in enumerate((gd1, gd2)):
        total = dpart[l, flat].astype(F32)
        for r in range(1, EP * DP):
            total += dense_got[l, r].astype(F32)
        vsum[l] = total.astype(BF)
        store(vsum.at[l], out)
    for copy in stores:
        copy.wait()


def solution(mesh):
    tok_spec = P(('dp', 'ep'), None)
    exp_spec = P('ep', None, None)
    layer_specs = (P(None, None), tok_spec, tok_spec, exp_spec, exp_spec, exp_spec)
    grad_specs = (P(('dp', 'ep'), None), P('ep', 'dp', None), P('ep', 'dp', None), P('ep', None, 'dp'))

    def local_step(tokens, dy_out, dense_w1, route_idx1, route_gate1, w_gate1, w_up1, w_down1, dense_w2, route_idx2, route_gate2, w_gate2, w_up2, w_down2):
        hbm = pl.BlockSpec(memory_space=pl.ANY)
        half = D // DP

        def sds(*shape):
            return jax.ShapeDtypeStruct(shape, BF)

        grads = (sds(32, D), sds(E_LOC, half, FF), sds(E_LOC, half, FF), sds(E_LOC, FF, half))
        vm = pltpu.VMEM
        got = (vm((2, E_LOC, half, FF), BF), vm((2, E_LOC, half, FF), BF), vm((2, E_LOC, FF, half), BF))
        parts = (vm((2, DP, E_LOC, half, FF), BF), vm((2, DP, E_LOC, half, FF), BF), vm((2, DP, E_LOC, FF, half), BF))
        dense = vm((2, EP * DP, 32, D), BF)
        on_chip = pl.BlockSpec(memory_space=pltpu.VMEM)
        dma = pltpu.SemaphoreType.DMA
        weights = [vm((D, D), BF), vm((E_LOC, TILES, D, 2 * LANES), BF), vm((E_LOC, FF, D), BF)]
        spread_buf = vm((EP, TOK, D), BF)
        ret_buf = vm((2 * EP - 1, TOK, D), BF)
        scratch = [vm((2, 2, TOK), jnp.int32), vm((2, 2, TOK), F32)]
        scratch += [vm((EP, 8, TOK), F32), spread_buf, spread_buf, spread_buf, spread_buf, ret_buf, ret_buf, ret_buf]
        scratch += weights + weights
        scratch += [vm((TOK, TOK), BF), vm((2, EP, 8, TOK), jnp.int32), vm((2, EP, 8, TOK), F32), vm((2, 8, TOK), jnp.int32)]
        scratch += [vm((2, TOK, EP * TOK), BF)]
        scratch += [vm((E_LOC, EP * CAP, D), BF)] * 3
        scratch += [vm((E_LOC, TILES, EP * CAP, 2 * LANES), F32), vm((E_LOC, EP * CAP, FF), BF), vm((E_LOC, TILES, EP * CAP, 2 * LANES), BF)]
        scratch += [spread_buf, vm((TOK, D), F32), vm((TOK, D), F32)]
        scratch += [dma((12,)), dma, dma((EP - 1,)), dma((2,)), dma((2, EP - 1, 2)), dma, dma((EP - 1, 2)),
                    dma((3,)), dma((2, 3)), dma((2,)), dma((2,))]
        results = pl.pallas_call(
            kernel,
            out_shape=(vm((TOK, D), BF),) + parts + got + (dense, dense),
            in_specs=[hbm] * 14,
            out_specs=(on_chip,) * 9,
            scratch_shapes=scratch,
            name='moe_backward',
            compiler_params=pltpu.CompilerParams(collective_id=0, has_side_effects=True, vmem_limit_bytes=VMEM_LIMIT),
        )(tokens, dy_out, route_idx1.T, route_idx2.T, route_gate1.T, route_gate2.T,
          dense_w1, w_gate1, w_up1, w_down1, dense_w2, w_gate2, w_up2, w_down2)
        return pl.pallas_call(
            finish,
            out_shape=(sds(TOK, D),) + grads + grads,
            in_specs=[on_chip] * 9,
            out_specs=(hbm,) * 9,
            scratch_shapes=list(got) + [vm((2, 32, D), BF), dma((9,))],
            name='finish',
            compiler_params=pltpu.CompilerParams(vmem_limit_bytes=16 * 1024 * 1024),
        )(*[pltpu.with_memory_space_constraint(r, pltpu.VMEM) for r in results])

    return jax.shard_map(local_step, mesh=mesh, in_specs=(tok_spec, tok_spec) + layer_specs + layer_specs,
                         out_specs=(tok_spec,) + grad_specs + grad_specs, check_vma=False)
```

```python
import jax
import jax.numpy as jnp
from jax import lax
from jax.experimental import pallas as pl
from jax.experimental.pallas import tpu as pltpu
from jax.sharding import PartitionSpec as P

MESH = pl.DeviceIdType.MESH
BF = jnp.bfloat16
F32 = jnp.float32
NN = ((1,), (0,))
NT = ((1,), (1,))
TN = ((0,), (0,))
EP = 4
DP = 2
E_LOC = 2
TOK = 512
CAP = 256
D = 256
FF = 896
LANES = 128
TILES = FF // LANES
VMEM_LIMIT = 60 * 1024 * 1024
X_IN, DY, Y_ONE, GM = range(4)
O_ONE, GR_TWO, GR_ONE = range(3)


def dot(a, b, dims=NN):
    return lax.dot_general(a, b, (dims, ((), ())), preferred_element_type=F32)


def place(k):
    return k + 3 * ((k + 3) // 4)


def unit(i):
    q = i // 2
    mid = (q + 1) // 2 % 2
    return mid * (1 + i % 2) + (1 - mid) * q, mid * (q - 1) + (1 - mid) * (i % 2)


def onehot(key_row):
    rows = lax.broadcasted_iota(jnp.int32, (CAP, TOK), 0)
    return jnp.where(rows == key_row, 1.0, 0.0).astype(BF)


def gate_column(key_row, gate_row):
    rows = lax.broadcasted_iota(jnp.int32, (CAP, TOK), 0)
    return jnp.sum(jnp.where(rows == key_row, gate_row, 0.0), axis=1, keepdims=True)


def kernel(tokens, dy, idx1, idx2, gate1, gate2, m1, g1, u1, w1, m2, g2, u2, w2,
           dx_out, got_g, got_u, got_w, dense_sum,
           ibuf, gbuf, rt, xin, dyb, yb, gmb, oret, grt2, grt1,
           vm1, vgu1, vw1, vm2, vgu2, vw2,
           tri, keys, gates, keyj, picks, x1, x2, gout, ab1, hb, gab, ub, p0, p1,
           wg, wu, wd, dpart, dense_got,
           loc_sem, rt_send, rt_recv, ag_send, ag_recv, ret_send, ret_recv, dp_send, dp_recv, all_send, all_recv):
    me = lax.axis_index('ep')
    dp = lax.axis_index('dp')
    flat = dp * EP + me
    other = 1 - dp

    barrier = pltpu.get_barrier_semaphore()
    def partner(k):
        return (me // 2 + k // 2) % 2 * 2 + (me + k) % 2

    for k in (1, 2):
        pl.semaphore_signal(barrier, inc=1, device_id={'ep': partner(k)}, device_id_type=MESH)
    pl.semaphore_signal(barrier, inc=1, device_id={'dp': other}, device_id_type=MESH)

    small = [(idx1, ibuf.at[0]), (idx2, ibuf.at[1]), (gate1, gbuf.at[0]), (gate2, gbuf.at[1]), (tokens, xin.at[0]), (dy, dyb.at[0])]
    small = [pltpu.make_async_copy(src, dst, loc_sem.at[n]) for n, (src, dst) in enumerate(small)]
    for copy in small:
        copy.start()

    def weight_copies(l, m, g, u, w, vm, vgu, vw):
        base = len(small) + 3 * l
        copies = [pltpu.make_async_copy(m, vm, loc_sem.at[base]), pltpu.make_async_copy(w, vw, loc_sem.at[base + 1])]
        for n in range(TILES):
            cols = pl.ds(n * LANES, LANES)
            for src, lanes in ((g, pl.ds(0, LANES)), (u, pl.ds(LANES, LANES))):
                copies.append(pltpu.make_async_copy(src.at[:, :, cols], vgu.at[:, n, :, lanes], loc_sem.at[base + 2]))
        whole = pltpu.make_async_copy(vgu, vgu, loc_sem.at[base + 2])
        return copies, copies[:2] + [whole]

    starts_one, waits_one = weight_copies(0, m1, g1, u1, w1, vm1, vgu1, vw1)
    starts_two, waits_two = weight_copies(1, m2, g2, u2, w2, vm2, vgu2, vw2)
    for copy in starts_one:
        copy.start()

    for copy in small[:4]:
        copy.wait()
    rt[0] = jnp.concatenate([ibuf[0].astype(F32), ibuf[1].astype(F32), gbuf[0], gbuf[1]], axis=0)
    small[4].wait()
    pl.semaphore_wait(barrier, 3)

    def remote(src, dst, send, recv, k):
        return pltpu.make_async_remote_copy(src_ref=src, dst_ref=dst, send_sem=send, recv_sem=recv,
                                            device_id={'ep': partner(k)}, device_id_type=MESH)

    def tell(k):
        return remote(rt.at[0], rt.at[k], rt_send, rt_recv.at[k - 1], k)

    def lane(phase):
        return 1 if phase == DY else 0

    def all_sent(buf, sem):
        remote(buf.at[pl.ds(1, EP - 1)], buf.at[pl.ds(1, EP - 1)], sem, sem, 1).wait_send()

    def half(h):
        return pl.ds(h * CAP, CAP)

    def ship(phase, buf, k, piece):
        rows = half(piece if k == 1 else 1 - piece)
        return remote(buf.at[0, rows], buf.at[k, rows], ag_send.at[lane(phase)], ag_recv.at[lane(phase), k - 1, piece], k)

    def relay(phase, buf, via):
        rows = half(via - 1)
        return remote(buf.at[via, rows], buf.at[3, rows], ag_send.at[lane(phase)], ag_recv.at[lane(phase), 2, via - 1], 3 - via)

    def spread(phase, buf):
        for piece in range(2):
            for k in (1, 2):
                ship(phase, buf, k, piece).start()

    def pass_on(phase, buf):
        for via in (1, 2):
            ship(phase, buf, via, 0).wait_recv()
            relay(phase, buf, via).start()

    def arrive(phase, buf, k):
        if k < 3:
            ship(phase, buf, k, 1).wait_recv()
        else:
            for via in (1, 2):
                relay(phase, buf, via).wait_recv()

    def giveback(phase, buf, k, el):
        rows = pl.ds(pl.multiple_of(el * CAP, CAP), CAP)
        return remote(buf.at[k, rows], buf.at[k + 3, rows], ret_send, ret_recv.at[k - 1, el], k)

    for k in (1, 2):
        tell(k).start()

    @pl.when(dp == 1)
    def _():
        small[5].wait()
        spread(DY, dyb)

    spread(X_IN, xin)
    for copy in starts_two:
        copy.start()

    tri[...] = jnp.where(lax.broadcasted_iota(jnp.int32, (TOK, TOK), 0) < lax.broadcasted_iota(jnp.int32, (TOK, TOK), 1), 1.0, 0.0).astype(BF)
    expert = lax.broadcasted_iota(jnp.int32, (E_LOC * EP, TOK), 0).astype(F32)

    def make_keys(k):
        info = rt[k]
        for l in range(2):
            hit0 = info[2 * l:2 * l + 1] == expert
            hit1 = info[2 * l + 1:2 * l + 2] == expert
            both = jnp.where(hit0, 1.0, jnp.where(hit1, 1.0, 0.0))
            rank = dot(both.astype(BF), tri[...]).astype(jnp.int32)
            keys[l, k] = jnp.where(both > 0.5, rank, -1)
            gates[l, k] = jnp.where(hit0, info[4 + 2 * l:5 + 2 * l], jnp.where(hit1, info[5 + 2 * l:6 + 2 * l], 0.0))
        return info

    info = make_keys(0)
    for j in range(2):
        keyj[j] = jnp.where(info[j:j + 1] == expert, keys[0, 0], -1)
    for copy in waits_one:
        copy.wait()

    def build_picks(*sources):
        slots = lax.broadcasted_iota(jnp.int32, (TOK, CAP), 1)
        for j, source in enumerate(sources):
            rows = [source[pl.ds(partner(k) * E_LOC + el, 1), :] for k in range(EP) for el in range(E_LOC)]
            cols = jnp.transpose(jnp.concatenate(rows, axis=0))
            for r in range(EP * E_LOC):
                picks[j, :, r * CAP:(r + 1) * CAP] = jnp.where(slots == cols[:, r:r + 1], 1.0, 0.0).astype(BF)

    def picked(j, ret, last):
        if last:
            return dot(picks[j, :, 3 * TOK:], ret[6])
        return dot(picks[j, :, :TOK], ret[0]) + dot(picks[j, :, TOK:3 * TOK], ret[4:6].reshape(2 * TOK, D))

    def silu_parts(a):
        sig = 0.5 * jnp.tanh(0.5 * a) + 0.5
        return sig, a * sig

    def groups():
        return [range(n, min(n + 2, TILES)) for n in range(0, TILES, 2)]

    def mixed(x, m):
        return (x.astype(F32) + dot(x, m[...])).astype(BF)

    def near_or_far(b):
        return ((b == 1, 1), (b == 1, 2), (b == 3, 3))

    def forward_one(b, carry):
        @pl.when(b == 0)
        def _():
            ub[0] = mixed(xin[0], vm1)

        @pl.when(b == 1)
        def _():
            build_picks(keyj.at[0], keyj.at[1])

            @pl.when(dp == 1)
            def _():
                pass_on(DY, dyb)

            tell(1).wait_recv()
            remote(rt.at[1], rt.at[3], rt_send, rt_recv.at[2], 2).start()
            pass_on(X_IN, xin)

        for ready, src in near_or_far(b):
            @pl.when(ready)
            def _():
                if src > 1:
                    tell(src).wait_recv()
                make_keys(src)
                arrive(X_IN, xin, src)
                ub[src] = mixed(xin[src], vm1)

        for k, el in (unit(2 * b), unit(2 * b + 1)):
            rows = pl.ds(pl.multiple_of(k * CAP, CAP), CAP)
            key = keys[0, k, pl.ds(me * E_LOC + el, 1), :]
            x = dot(onehot(key), ub[k]).astype(BF)
            x1[el, rows] = x
            out = jnp.zeros((CAP, D), F32)
            for group in groups():
                h = []
                for n in group:
                    ab = dot(x, vgu1[el, n])
                    ab1[el, n, rows] = ab
                    h.append((silu_parts(ab[:, :LANES])[1] * ab[:, LANES:]).astype(BF))
                out += dot(jnp.concatenate(h, axis=1), vw1[el, group[0] * LANES:(group[-1] + 1) * LANES])
            oret[k, pl.ds(pl.multiple_of(el * CAP, CAP), CAP)] = out.astype(BF)

        returns(b, O_ONE, oret)
        return carry

    def returns(b, phase, ret):
        @pl.when(b > 0)
        def _():
            for k, el in (unit(2 * b), unit(2 * b + 1)):
                giveback(phase, ret, k, el).start()

    lax.fori_loop(0, EP, forward_one, 0)

    @pl.when(dp == 0)
    def _():
        small[5].wait()
        spread(DY, dyb)

    for copy in waits_two:
        copy.wait()

    def collect(phase, ret, ks):
        for k in ks:
            for el in range(E_LOC):
                giveback(phase, ret, k, el).wait_recv()

    collect(O_ONE, oret, (1, 2))
    p0[...] = picked(0, oret, False)
    p1[...] = picked(1, oret, False)
    gcol0 = jnp.transpose(jnp.broadcast_to(rt[0, 4:5], (8, TOK)))[:, :1]
    gcol1 = jnp.transpose(jnp.broadcast_to(rt[0, 5:6], (8, TOK)))[:, :1]
    collect(O_ONE, oret, (3,))
    out0 = p0[...] + picked(0, oret, True)
    out1 = p1[...] + picked(1, oret, True)
    yb[0] = (ub[0].astype(F32) + (gcol0 * out0 + gcol1 * out1)).astype(BF)
    all_sent(xin, ag_send.at[0])
    spread(Y_ONE, yb)

    def expert_backward(k, el, first, vgu, vw, ret):
        rows = pl.ds(pl.multiple_of(k * CAP, CAP), CAP)
        go = gout[el, rows]
        back = jnp.zeros((CAP, D), F32)
        for group in groups():
            cols = slice(group[0] * LANES, (group[-1] + 1) * LANES)
            grad_h = dot(go, vw[el, cols], NT).astype(BF).astype(F32)
            for n in group:
                ab = first(n)
                a, b = ab[:, :LANES], ab[:, LANES:]
                dh = grad_h[:, (n - group[0]) * LANES:(n - group[0] + 1) * LANES]
                sig, s = silu_parts(a)
                hb[el, rows, n * LANES:(n + 1) * LANES] = (s * b).astype(BF)
                grad_a = (dh * b * (sig + s * (1.0 - sig))).astype(BF)
                grad_b = (dh * s).astype(BF)
                grads = jnp.concatenate([grad_a, grad_b], axis=1)
                gab[el, n, rows] = grads
                back += dot(grads, vgu[el, n], NT)
        ret[k, pl.ds(pl.multiple_of(el * CAP, CAP), CAP)] = back.astype(BF)

    all_sent(oret, ret_send)

    def layer_two(b, carry):
        @pl.when(b == 0)
        def _():
            ub[0] = mixed(yb[0], vm2)

        @pl.when(b == 1)
        def _():
            build_picks(keys.at[1, 0])

            @pl.when(dp == 0)
            def _():
                pass_on(DY, dyb)

            pass_on(Y_ONE, yb)

        for ready, src in near_or_far(b):
            @pl.when(ready)
            def _():
                arrive(DY, dyb, src)
                arrive(Y_ONE, yb, src)
                ub[src] = mixed(yb[src], vm2)

        for k, el in (unit(2 * b), unit(2 * b + 1)):
            rows = pl.ds(pl.multiple_of(k * CAP, CAP), CAP)
            e = pl.ds(me * E_LOC + el, 1)
            key = keys[1, k, e, :]
            pick = onehot(key)
            x = dot(pick, ub[k]).astype(BF)
            x2[el, rows] = x
            gout[el, rows] = (dot(pick, dyb[k]) * gate_column(key, gates[1, k, e, :])).astype(BF)
            expert_backward(k, el, lambda n: dot(x, vgu2[el, n]), vgu2, vw2, grt2)

        returns(b, GR_TWO, grt2)
        return carry

    lax.fori_loop(0, EP, layer_two, 0)

    stacks = ((wg, got_g), (wu, got_u), (wd, got_w))

    def pairs(l):
        return [pltpu.make_async_remote_copy(src_ref=part.at[l, other], dst_ref=got.at[l], send_sem=dp_send.at[n],
                                             recv_sem=dp_recv.at[l, n], device_id={'dp': other}, device_id_type=MESH)
                for n, (part, got) in enumerate(stacks)]

    def weight_grads(l, x_all, el):
        half_d = D // DP
        x = x_all[el]
        down = dot(hb[el], gout[el], TN).astype(BF)
        for d in range(DP):
            wd[l, d, el] = down[:, d * half_d:(d + 1) * half_d]

        for n in range(TILES):
            cols = slice(n * LANES, (n + 1) * LANES)
            both = dot(x, gab[el, n], TN).astype(BF)
            for d in range(DP):
                rows = slice(d * half_d, (d + 1) * half_d)
                wg[l, d, el, :, cols] = both[rows, :LANES]
                wu[l, d, el, :, cols] = both[rows, LANES:]

    def send_weight_grads(l):
        if l == 0:
            for copy in pairs(1):
                copy.wait_send()
        for copy in pairs(l):
            copy.start()

    weight_grads(1, x2, 0)

    def backward_combine(phase, ret, grad_y):
        collect(phase, ret, (1, 2))
        p0[...] = picked(0, ret, False)
        collect(phase, ret, (3,))
        return (grad_y.astype(F32) + (p0[...] + picked(0, ret, True))).astype(BF)

    def grad_input(grad_mixed, m):
        return (grad_mixed.astype(F32) + dot(grad_mixed, m[...], NT)).astype(BF)

    def dense_copies(l):
        copies = []
        for r in range(1, EP * DP):
            peer = (flat + r) % (EP * DP)
            copies.append(pltpu.make_async_remote_copy(
                src_ref=dpart.at[l, peer], dst_ref=dense_got.at[l, r], send_sem=all_send.at[l], recv_sem=all_recv.at[l],
                device_id={'ep': peer % EP, 'dp': peer // EP}, device_id_type=MESH))
        return copies

    def dense_grad(l, x, grad_mixed):
        part = dot(x, grad_mixed, TN).astype(BF)
        for q in range(EP * DP):
            dpart[l, q] = part[q * 32:(q + 1) * 32]
        for copy in dense_copies(l):
            copy.start()

    grad_mixed = backward_combine(GR_TWO, grt2, dyb[0])
    gmb[0] = grad_input(grad_mixed, vm2)
    all_sent(yb, ag_send.at[0])
    spread(GM, gmb)
    weight_grads(1, x2, 1)
    send_weight_grads(1)
    dense_grad(1, yb[0], grad_mixed)

    all_sent(grt2, ret_send)

    def backward_one(b, carry):
        @pl.when(b == 0)
        def _():
            build_picks(keys.at[0, 0])
            pass_on(GM, gmb)

        for ready, src in near_or_far(b):
            @pl.when(ready)
            def _():
                arrive(GM, gmb, src)

        for k, el in (unit(2 * b), unit(2 * b + 1)):
            rows = pl.ds(pl.multiple_of(k * CAP, CAP), CAP)
            e = pl.ds(me * E_LOC + el, 1)
            key = keys[0, k, e, :]
            gout[el, rows] = (dot(onehot(key), gmb[k]) * gate_column(key, gates[0, k, e, :])).astype(BF)
            expert_backward(k, el, lambda n: ab1[el, n, rows], vgu1, vw1, grt1)

        returns(b, GR_ONE, grt1)
        return carry

    lax.fori_loop(0, EP, backward_one, 0)
    weight_grads(0, x1, 0)
    weight_grads(0, x1, 1)
    send_weight_grads(0)
    grad_mixed = backward_combine(GR_ONE, grt1, gmb[0])
    dense_grad(0, xin[0], grad_mixed)
    dx_out[...] = grad_input(grad_mixed, vm1)

    all_sent(rt, rt_send)
    all_sent(dyb, ag_send.at[1])
    all_sent(gmb, ag_send.at[0])
    all_sent(grt1, ret_send)
    for copy in pairs(1):
        copy.wait_recv()
    for copy in pairs(0):
        copy.wait()
    for l in range(2):
        for part, got in stacks:
            got[l] = (part[l, dp].astype(F32) + got[l].astype(F32)).astype(BF)
    for l in range(2):
        whole = pl.ds(1, EP * DP - 1)
        pltpu.make_async_remote_copy(src_ref=dpart.at[l, whole], dst_ref=dense_got.at[l, whole], send_sem=all_send.at[l], recv_sem=all_recv.at[l],
                                     device_id={'dp': other}, device_id_type=MESH).wait()
        total = dpart[l, flat].astype(F32)
        for r in range(1, EP * DP):
            total += dense_got[l, r].astype(F32)
        dense_sum[l] = total.astype(BF)


def finish(dx, got_g, got_u, got_w, dense_sum, dx_out, gd1, gg1, gu1, gw1, gd2, gg2, gu2, gw2, out_sem):
    moves = [(got_g.at[0], gg1), (got_u.at[0], gu1), (got_w.at[0], gw1), (got_g.at[1], gg2), (got_u.at[1], gu2), (got_w.at[1], gw2),
             (dx, dx_out), (dense_sum.at[0], gd1), (dense_sum.at[1], gd2)]
    moves = [pltpu.make_async_copy(src, dst, out_sem.at[n]) for n, (src, dst) in enumerate(moves)]
    for copy in moves:
        copy.start()
    for copy in moves:
        copy.wait()


def solution(mesh):
    tok_spec = P(('dp', 'ep'), None)
    exp_spec = P('ep', None, None)
    layer_specs = (P(None, None), tok_spec, tok_spec, exp_spec, exp_spec, exp_spec)
    grad_specs = (P(('dp', 'ep'), None), P('ep', 'dp', None), P('ep', 'dp', None), P('ep', None, 'dp'))

    def local_step(tokens, dy_out, dense_w1, route_idx1, route_gate1, w_gate1, w_up1, w_down1, dense_w2, route_idx2, route_gate2, w_gate2, w_up2, w_down2):
        hbm = pl.BlockSpec(memory_space=pl.ANY)
        half = D // DP

        def sds(*shape):
            return jax.ShapeDtypeStruct(shape, BF)

        grads = (sds(32, D), sds(E_LOC, half, FF), sds(E_LOC, half, FF), sds(E_LOC, FF, half))
        vm = pltpu.VMEM
        got = (vm((2, E_LOC, half, FF), BF), vm((2, E_LOC, half, FF), BF), vm((2, E_LOC, FF, half), BF))
        parts = (vm((2, DP, E_LOC, half, FF), BF), vm((2, DP, E_LOC, half, FF), BF), vm((2, DP, E_LOC, FF, half), BF))
        dense = vm((2, EP * DP, 32, D), BF)
        on_chip = pl.BlockSpec(memory_space=pltpu.VMEM)
        dma = pltpu.SemaphoreType.DMA
        weights = [vm((D, D), BF), vm((E_LOC, TILES, D, 2 * LANES), BF), vm((E_LOC, FF, D), BF)]
        spread_buf = vm((EP, TOK, D), BF)
        ret_buf = vm((2 * EP - 1, TOK, D), BF)
        scratch = [vm((2, 2, TOK), jnp.int32), vm((2, 2, TOK), F32)]
        scratch += [vm((EP, 8, TOK), F32), spread_buf, spread_buf, spread_buf, spread_buf, ret_buf, ret_buf, ret_buf]
        scratch += weights + weights
        scratch += [vm((TOK, TOK), BF), vm((2, EP, 8, TOK), jnp.int32), vm((2, EP, 8, TOK), F32), vm((2, 8, TOK), jnp.int32)]
        scratch += [vm((2, TOK, EP * TOK), BF)]
        scratch += [vm((E_LOC, EP * CAP, D), BF)] * 3
        scratch += [vm((E_LOC, TILES, EP * CAP, 2 * LANES), F32), vm((E_LOC, EP * CAP, FF), BF), vm((E_LOC, TILES, EP * CAP, 2 * LANES), BF)]
        scratch += [spread_buf, vm((TOK, D), F32), vm((TOK, D), F32)]
        scratch += list(parts) + [dense, dense]
        scratch += [dma((12,)), dma, dma((EP - 1,)), dma((2,)), dma((2, EP - 1, 2)), dma, dma((EP - 1, 2)),
                    dma((3,)), dma((2, 3)), dma((2,)), dma((2,))]
        results = pl.pallas_call(
            kernel,
            out_shape=(vm((TOK, D), BF),) + got + (vm((2, 32, D), BF),),
            in_specs=[hbm] * 14,
            out_specs=(on_chip,) * 5,
            scratch_shapes=scratch,
            name='moe_backward',
            compiler_params=pltpu.CompilerParams(collective_id=0, has_side_effects=True, vmem_limit_bytes=VMEM_LIMIT),
        )(tokens, dy_out, route_idx1.T, route_idx2.T, route_gate1.T, route_gate2.T,
          dense_w1, w_gate1, w_up1, w_down1, dense_w2, w_gate2, w_up2, w_down2)
        return pl.pallas_call(
            finish,
            out_shape=(sds(TOK, D),) + grads + grads,
            in_specs=[on_chip] * 5,
            out_specs=(hbm,) * 9,
            scratch_shapes=[dma((9,))],
            name='finish',
            compiler_params=pltpu.CompilerParams(vmem_limit_bytes=16 * 1024 * 1024),
        )(*[pltpu.with_memory_space_constraint(r, pltpu.VMEM) for r in results])

    return jax.shard_map(local_step, mesh=mesh, in_specs=(tok_spec, tok_spec) + layer_specs + layer_specs,
                         out_specs=(tok_spec,) + grad_specs + grad_specs, check_vma=False)
```

```python
import jax
import jax.numpy as jnp
from jax import lax
from jax.experimental import pallas as pl
from jax.experimental.pallas import tpu as pltpu
from jax.sharding import PartitionSpec as P

MESH = pl.DeviceIdType.MESH
BF = jnp.bfloat16
F32 = jnp.float32
NN = ((1,), (0,))
NT = ((1,), (1,))
TN = ((0,), (0,))
EP = 4
DP = 2
E_LOC = 2
TOK = 512
CAP = 256
D = 256
FF = 896
LANES = 128
TILES = FF // LANES
VMEM_LIMIT = 60 * 1024 * 1024
X_IN, DY, Y_ONE, GM = range(4)
O_ONE, GR_TWO, GR_ONE = range(3)


def dot(a, b, dims=NN):
    return lax.dot_general(a, b, (dims, ((), ())), preferred_element_type=F32)


def place(k):
    return k + 3 * ((k + 3) // 4)


def unit(i):
    q = i // 2
    mid = (q + 1) // 2 % 2
    return mid * (1 + i % 2) + (1 - mid) * q, mid * (q - 1) + (1 - mid) * (i % 2)


def onehot(key_row):
    rows = lax.broadcasted_iota(jnp.int32, (CAP, TOK), 0)
    return jnp.where(rows == key_row, 1.0, 0.0).astype(BF)


def gate_column(key_row, gate_row):
    rows = lax.broadcasted_iota(jnp.int32, (CAP, TOK), 0)
    return jnp.sum(jnp.where(rows == key_row, gate_row, 0.0), axis=1, keepdims=True)


def kernel(tokens, dy, idx1, idx2, gate1, gate2, m1, g1, u1, w1, m2, g2, u2, w2,
           dx_out, got_g, got_u, got_w, dense_sum,
           ibuf, gbuf, rt, xin, dyb, yb, gmb, oret, grt2, grt1,
           vm1, vgu1, vw1, vm2, vgu2, vw2,
           tri, keys, gates, keyj, picks, x1, x2, gout, ab1, hb, gab, ub, p0, p1,
           wg, wu, wd, dpart, dense_got,
           loc_sem, rt_send, rt_recv, ag_send, ag_recv, ret_send, ret_recv, dp_send, dp_recv, all_send, all_recv):
    me = lax.axis_index('ep')
    dp = lax.axis_index('dp')
    flat = dp * EP + me
    other = 1 - dp

    barrier = pltpu.get_barrier_semaphore()
    def partner(k):
        return (me // 2 + k // 2) % 2 * 2 + (me + k) % 2

    for k in (1, 2):
        pl.semaphore_signal(barrier, inc=1, device_id={'ep': partner(k)}, device_id_type=MESH)
    pl.semaphore_signal(barrier, inc=1, device_id={'dp': other}, device_id_type=MESH)

    small = [(idx1, ibuf.at[0]), (idx2, ibuf.at[1]), (gate1, gbuf.at[0]), (gate2, gbuf.at[1]), (tokens, xin.at[0]), (dy, dyb.at[0])]
    small = [pltpu.make_async_copy(src, dst, loc_sem.at[n]) for n, (src, dst) in enumerate(small)]
    for copy in small:
        copy.start()

    def weight_copies(l, m, g, u, w, vm, vgu, vw):
        base = len(small) + 3 * l
        copies = [pltpu.make_async_copy(m, vm, loc_sem.at[base]), pltpu.make_async_copy(w, vw, loc_sem.at[base + 1])]
        for n in range(TILES):
            cols = pl.ds(n * LANES, LANES)
            for src, lanes in ((g, pl.ds(0, LANES)), (u, pl.ds(LANES, LANES))):
                copies.append(pltpu.make_async_copy(src.at[:, :, cols], vgu.at[:, n, :, lanes], loc_sem.at[base + 2]))
        whole = pltpu.make_async_copy(vgu, vgu, loc_sem.at[base + 2])
        return copies, copies[:2] + [whole]

    starts_one, waits_one = weight_copies(0, m1, g1, u1, w1, vm1, vgu1, vw1)
    starts_two, waits_two = weight_copies(1, m2, g2, u2, w2, vm2, vgu2, vw2)
    for copy in starts_one:
        copy.start()

    for copy in small[:4]:
        copy.wait()
    rt[0] = jnp.concatenate([ibuf[0].astype(F32), ibuf[1].astype(F32), gbuf[0], gbuf[1]], axis=0)
    small[4].wait()
    pl.semaphore_wait(barrier, 3)

    def remote(src, dst, send, recv, k):
        return pltpu.make_async_remote_copy(src_ref=src, dst_ref=dst, send_sem=send, recv_sem=recv,
                                            device_id={'ep': partner(k)}, device_id_type=MESH)

    def tell(k):
        return remote(rt.at[0], rt.at[k], rt_send, rt_recv.at[k - 1], k)

    def lane(phase):
        return 1 if phase == DY else 0

    def all_sent(buf, sem):
        remote(buf.at[pl.ds(1, EP - 1)], buf.at[pl.ds(1, EP - 1)], sem, sem, 1).wait_send()

    def half(h):
        return pl.ds(h * CAP, CAP)

    def ship(phase, buf, k, piece):
        rows = half(piece if k == 1 else 1 - piece)
        return remote(buf.at[0, rows], buf.at[k, rows], ag_send.at[lane(phase)], ag_recv.at[lane(phase), k - 1, piece], k)

    def relay(phase, buf, via):
        rows = half(via - 1)
        return remote(buf.at[via, rows], buf.at[3, rows], ag_send.at[lane(phase)], ag_recv.at[lane(phase), 2, via - 1], 3 - via)

    def spread(phase, buf):
        for piece in range(2):
            for k in (1, 2):
                ship(phase, buf, k, piece).start()

    def pass_on(phase, buf):
        for via in (1, 2):
            ship(phase, buf, via, 0).wait_recv()
            relay(phase, buf, via).start()

    def arrive(phase, buf, k):
        if k < 3:
            ship(phase, buf, k, 1).wait_recv()
        else:
            for via in (1, 2):
                relay(phase, buf, via).wait_recv()

    def giveback(phase, buf, k, el):
        rows = pl.ds(pl.multiple_of(el * CAP, CAP), CAP)
        return remote(buf.at[k, rows], buf.at[k + 3, rows], ret_send, ret_recv.at[k - 1, el], k)

    for k in (1, 2):
        tell(k).start()

    @pl.when(dp == 1)
    def _():
        small[5].wait()
        spread(DY, dyb)

    spread(X_IN, xin)
    for copy in starts_two:
        copy.start()

    tri[...] = jnp.where(lax.broadcasted_iota(jnp.int32, (TOK, TOK), 0) < lax.broadcasted_iota(jnp.int32, (TOK, TOK), 1), 1.0, 0.0).astype(BF)
    expert = lax.broadcasted_iota(jnp.int32, (E_LOC * EP, TOK), 0).astype(F32)

    def make_keys(k):
        info = rt[k]
        for l in range(2):
            hit0 = info[2 * l:2 * l + 1] == expert
            hit1 = info[2 * l + 1:2 * l + 2] == expert
            both = jnp.where(hit0, 1.0, jnp.where(hit1, 1.0, 0.0))
            rank = dot(both.astype(BF), tri[...]).astype(jnp.int32)
            keys[l, k] = jnp.where(both > 0.5, rank, -1)
            gates[l, k] = jnp.where(hit0, info[4 + 2 * l:5 + 2 * l], jnp.where(hit1, info[5 + 2 * l:6 + 2 * l], 0.0))
        return info

    info = make_keys(0)
    for j in range(2):
        keyj[j] = jnp.where(info[j:j + 1] == expert, keys[0, 0], -1)
    for copy in waits_one:
        copy.wait()

    def build_picks(*sources):
        slots = lax.broadcasted_iota(jnp.int32, (TOK, CAP), 1)
        for j, source in enumerate(sources):
            rows = [source[pl.ds(partner(k) * E_LOC + el, 1), :] for k in range(EP) for el in range(E_LOC)]
            cols = jnp.transpose(jnp.concatenate(rows, axis=0))
            for r in range(EP * E_LOC):
                picks[j, :, r * CAP:(r + 1) * CAP] = jnp.where(slots == cols[:, r:r + 1], 1.0, 0.0).astype(BF)

    def picked(j, ret, last):
        if last:
            rows = slice((last - 1) * CAP, last * CAP)
            return dot(picks[j, :, 3 * TOK + (last - 1) * CAP:3 * TOK + last * CAP], ret[6, rows])
        return dot(picks[j, :, :TOK], ret[0]) + dot(picks[j, :, TOK:3 * TOK], ret[4:6].reshape(2 * TOK, D))

    def silu_parts(a):
        sig = 0.5 * jnp.tanh(0.5 * a) + 0.5
        return sig, a * sig

    def groups():
        return [range(n, min(n + 2, TILES)) for n in range(0, TILES, 2)]

    def mixed(x, m):
        return (x.astype(F32) + dot(x, m[...])).astype(BF)

    def near_or_far(b):
        return ((b == 1, 1), (b == 1, 2), (b == 3, 3))

    def forward_one(b, carry):
        @pl.when(b == 0)
        def _():
            ub[0] = mixed(xin[0], vm1)

        @pl.when(b == 1)
        def _():
            build_picks(keyj.at[0], keyj.at[1])

            @pl.when(dp == 1)
            def _():
                pass_on(DY, dyb)

            tell(1).wait_recv()
            remote(rt.at[1], rt.at[3], rt_send, rt_recv.at[2], 2).start()
            pass_on(X_IN, xin)

        for ready, src in near_or_far(b):
            @pl.when(ready)
            def _():
                if src > 1:
                    tell(src).wait_recv()
                make_keys(src)
                arrive(X_IN, xin, src)
                ub[src] = mixed(xin[src], vm1)

        for k, el in (unit(2 * b), unit(2 * b + 1)):
            rows = pl.ds(pl.multiple_of(k * CAP, CAP), CAP)
            key = keys[0, k, pl.ds(me * E_LOC + el, 1), :]
            x = dot(onehot(key), ub[k]).astype(BF)
            x1[el, rows] = x
            out = jnp.zeros((CAP, D), F32)
            for group in groups():
                h = []
                for n in group:
                    ab = dot(x, vgu1[el, n])
                    ab1[el, n, rows] = ab
                    h.append((silu_parts(ab[:, :LANES])[1] * ab[:, LANES:]).astype(BF))
                out += dot(jnp.concatenate(h, axis=1), vw1[el, group[0] * LANES:(group[-1] + 1) * LANES])
            oret[k, pl.ds(pl.multiple_of(el * CAP, CAP), CAP)] = out.astype(BF)

        returns(b, O_ONE, oret)
        return carry

    def returns(b, phase, ret):
        @pl.when(b > 0)
        def _():
            for k, el in (unit(2 * b), unit(2 * b + 1)):
                giveback(phase, ret, k, el).start()

    lax.fori_loop(0, EP, forward_one, 0)

    @pl.when(dp == 0)
    def _():
        small[5].wait()
        spread(DY, dyb)

    for copy in waits_two:
        copy.wait()

    def collect(phase, ret, ks, els=range(E_LOC)):
        for k in ks:
            for el in els:
                giveback(phase, ret, k, el).wait_recv()

    collect(O_ONE, oret, (1, 2))
    p0[...] = picked(0, oret, 0)
    p1[...] = picked(1, oret, 0)
    gcol0 = jnp.transpose(jnp.broadcast_to(rt[0, 4:5], (8, TOK)))[:, :1]
    gcol1 = jnp.transpose(jnp.broadcast_to(rt[0, 5:6], (8, TOK)))[:, :1]
    collect(O_ONE, oret, (3,), (0,))
    p0[...] += picked(0, oret, 1)
    p1[...] += picked(1, oret, 1)
    collect(O_ONE, oret, (3,), (1,))
    out0 = p0[...] + picked(0, oret, 2)
    out1 = p1[...] + picked(1, oret, 2)
    yb[0] = (ub[0].astype(F32) + (gcol0 * out0 + gcol1 * out1)).astype(BF)
    @pl.when(dp == 1)
    def _():
        build_picks(keys.at[1, 0])
        ub[0] = mixed(yb[0], vm2)

    all_sent(xin, ag_send.at[0])
    spread(Y_ONE, yb)

    def expert_backward(k, el, first, vgu, vw, ret):
        rows = pl.ds(pl.multiple_of(k * CAP, CAP), CAP)
        go = gout[el, rows]
        back = jnp.zeros((CAP, D), F32)
        for group in groups():
            cols = slice(group[0] * LANES, (group[-1] + 1) * LANES)
            grad_h = dot(go, vw[el, cols], NT).astype(BF).astype(F32)
            for n in group:
                ab = first(n)
                a, b = ab[:, :LANES], ab[:, LANES:]
                dh = grad_h[:, (n - group[0]) * LANES:(n - group[0] + 1) * LANES]
                sig, s = silu_parts(a)
                hb[el, rows, n * LANES:(n + 1) * LANES] = (s * b).astype(BF)
                grad_a = (dh * b * (sig + s * (1.0 - sig))).astype(BF)
                grad_b = (dh * s).astype(BF)
                grads = jnp.concatenate([grad_a, grad_b], axis=1)
                gab[el, n, rows] = grads
                back += dot(grads, vgu[el, n], NT)
        ret[k, pl.ds(pl.multiple_of(el * CAP, CAP), CAP)] = back.astype(BF)

    all_sent(oret, ret_send)

    def layer_two(b, carry):
        @pl.when(b == 0)
        def _():
            @pl.when(dp == 0)
            def _():
                ub[0] = mixed(yb[0], vm2)

        @pl.when(b == 1)
        def _():
            @pl.when(dp == 0)
            def _():
                build_picks(keys.at[1, 0])

            @pl.when(dp == 0)
            def _():
                pass_on(DY, dyb)

            pass_on(Y_ONE, yb)

        for ready, src in near_or_far(b):
            @pl.when(ready)
            def _():
                arrive(DY, dyb, src)
                arrive(Y_ONE, yb, src)
                ub[src] = mixed(yb[src], vm2)

        for k, el in (unit(2 * b), unit(2 * b + 1)):
            rows = pl.ds(pl.multiple_of(k * CAP, CAP), CAP)
            e = pl.ds(me * E_LOC + el, 1)
            key = keys[1, k, e, :]
            pick = onehot(key)
            x = dot(pick, ub[k]).astype(BF)
            x2[el, rows] = x
            gout[el, rows] = (dot(pick, dyb[k]) * gate_column(key, gates[1, k, e, :])).astype(BF)
            expert_backward(k, el, lambda n: dot(x, vgu2[el, n]), vgu2, vw2, grt2)

        returns(b, GR_TWO, grt2)
        return carry

    lax.fori_loop(0, EP, layer_two, 0)

    stacks = ((wg, got_g), (wu, got_u), (wd, got_w))

    def pairs(l):
        return [pltpu.make_async_remote_copy(src_ref=part.at[l, other], dst_ref=got.at[l], send_sem=dp_send.at[n],
                                             recv_sem=dp_recv.at[l, n], device_id={'dp': other}, device_id_type=MESH)
                for n, (part, got) in enumerate(stacks)]

    def weight_grads(l, x_all, el):
        half_d = D // DP
        x = x_all[el]
        down = dot(hb[el], gout[el], TN).astype(BF)
        for d in range(DP):
            wd[l, d, el] = down[:, d * half_d:(d + 1) * half_d]

        for n in range(TILES):
            cols = slice(n * LANES, (n + 1) * LANES)
            both = dot(x, gab[el, n], TN).astype(BF)
            for d in range(DP):
                rows = slice(d * half_d, (d + 1) * half_d)
                wg[l, d, el, :, cols] = both[rows, :LANES]
                wu[l, d, el, :, cols] = both[rows, LANES:]

    def send_weight_grads(l):
        if l == 0:
            for copy in pairs(1):
                copy.wait_send()
        for copy in pairs(l):
            copy.start()

    weight_grads(1, x2, 0)

    def backward_combine(phase, ret, grad_y):
        collect(phase, ret, (1, 2))
        p0[...] = picked(0, ret, 0)
        collect(phase, ret, (3,), (0,))
        p0[...] += picked(0, ret, 1)
        collect(phase, ret, (3,), (1,))
        return (grad_y.astype(F32) + (p0[...] + picked(0, ret, 2))).astype(BF)

    def grad_input(grad_mixed, m):
        return (grad_mixed.astype(F32) + dot(grad_mixed, m[...], NT)).astype(BF)

    def dense_copies(l):
        copies = []
        for r in range(1, EP * DP):
            peer = (flat + r) % (EP * DP)
            copies.append(pltpu.make_async_remote_copy(
                src_ref=dpart.at[l, peer], dst_ref=dense_got.at[l, r], send_sem=all_send.at[l], recv_sem=all_recv.at[l],
                device_id={'ep': peer % EP, 'dp': peer // EP}, device_id_type=MESH))
        return copies

    def dense_grad(l, x, grad_mixed):
        part = dot(x, grad_mixed, TN).astype(BF)
        for q in range(EP * DP):
            dpart[l, q] = part[q * 32:(q + 1) * 32]
        for copy in dense_copies(l):
            copy.start()

    grad_mixed = backward_combine(GR_TWO, grt2, dyb[0])
    gmb[0] = grad_input(grad_mixed, vm2)
    all_sent(yb, ag_send.at[0])
    spread(GM, gmb)
    weight_grads(1, x2, 1)
    send_weight_grads(1)
    dense_grad(1, yb[0], grad_mixed)

    all_sent(grt2, ret_send)

    def backward_one(b, carry):
        @pl.when(b == 0)
        def _():
            build_picks(keys.at[0, 0])
            pass_on(GM, gmb)

        for ready, src in near_or_far(b):
            @pl.when(ready)
            def _():
                arrive(GM, gmb, src)

        for k, el in (unit(2 * b), unit(2 * b + 1)):
            rows = pl.ds(pl.multiple_of(k * CAP, CAP), CAP)
            e = pl.ds(me * E_LOC + el, 1)
            key = keys[0, k, e, :]
            gout[el, rows] = (dot(onehot(key), gmb[k]) * gate_column(key, gates[0, k, e, :])).astype(BF)
            expert_backward(k, el, lambda n: ab1[el, n, rows], vgu1, vw1, grt1)

        returns(b, GR_ONE, grt1)
        return carry

    lax.fori_loop(0, EP, backward_one, 0)
    weight_grads(0, x1, 0)
    weight_grads(0, x1, 1)
    send_weight_grads(0)
    grad_mixed = backward_combine(GR_ONE, grt1, gmb[0])
    dense_grad(0, xin[0], grad_mixed)
    dx_out[...] = grad_input(grad_mixed, vm1)

    all_sent(rt, rt_send)
    all_sent(dyb, ag_send.at[1])
    all_sent(gmb, ag_send.at[0])
    all_sent(grt1, ret_send)
    for copy in pairs(1):
        copy.wait_recv()
    for copy in pairs(0):
        copy.wait()
    for l in range(2):
        for part, got in stacks:
            got[l] = (part[l, dp].astype(F32) + got[l].astype(F32)).astype(BF)
    for l in range(2):
        whole = pl.ds(1, EP * DP - 1)
        pltpu.make_async_remote_copy(src_ref=dpart.at[l, whole], dst_ref=dense_got.at[l, whole], send_sem=all_send.at[l], recv_sem=all_recv.at[l],
                                     device_id={'dp': other}, device_id_type=MESH).wait()
        total = dpart[l, flat].astype(F32)
        for r in range(1, EP * DP):
            total += dense_got[l, r].astype(F32)
        dense_sum[l] = total.astype(BF)


def finish(dx, got_g, got_u, got_w, dense_sum, dx_out, gd1, gg1, gu1, gw1, gd2, gg2, gu2, gw2, out_sem):
    moves = [(got_g.at[0], gg1), (got_u.at[0], gu1), (got_w.at[0], gw1), (got_g.at[1], gg2), (got_u.at[1], gu2), (got_w.at[1], gw2),
             (dx, dx_out), (dense_sum.at[0], gd1), (dense_sum.at[1], gd2)]
    moves = [pltpu.make_async_copy(src, dst, out_sem.at[n]) for n, (src, dst) in enumerate(moves)]
    for copy in moves:
        copy.start()
    for copy in moves:
        copy.wait()


def solution(mesh):
    tok_spec = P(('dp', 'ep'), None)
    exp_spec = P('ep', None, None)
    layer_specs = (P(None, None), tok_spec, tok_spec, exp_spec, exp_spec, exp_spec)
    grad_specs = (P(('dp', 'ep'), None), P('ep', 'dp', None), P('ep', 'dp', None), P('ep', None, 'dp'))

    def local_step(tokens, dy_out, dense_w1, route_idx1, route_gate1, w_gate1, w_up1, w_down1, dense_w2, route_idx2, route_gate2, w_gate2, w_up2, w_down2):
        hbm = pl.BlockSpec(memory_space=pl.ANY)
        half = D // DP

        def sds(*shape):
            return jax.ShapeDtypeStruct(shape, BF)

        grads = (sds(32, D), sds(E_LOC, half, FF), sds(E_LOC, half, FF), sds(E_LOC, FF, half))
        vm = pltpu.VMEM
        got = (vm((2, E_LOC, half, FF), BF), vm((2, E_LOC, half, FF), BF), vm((2, E_LOC, FF, half), BF))
        parts = (vm((2, DP, E_LOC, half, FF), BF), vm((2, DP, E_LOC, half, FF), BF), vm((2, DP, E_LOC, FF, half), BF))
        dense = vm((2, EP * DP, 32, D), BF)
        on_chip = pl.BlockSpec(memory_space=pltpu.VMEM)
        dma = pltpu.SemaphoreType.DMA
        weights = [vm((D, D), BF), vm((E_LOC, TILES, D, 2 * LANES), BF), vm((E_LOC, FF, D), BF)]
        spread_buf = vm((EP, TOK, D), BF)
        ret_buf = vm((2 * EP - 1, TOK, D), BF)
        scratch = [vm((2, 2, TOK), jnp.int32), vm((2, 2, TOK), F32)]
        scratch += [vm((EP, 8, TOK), F32), spread_buf, spread_buf, spread_buf, spread_buf, ret_buf, ret_buf, ret_buf]
        scratch += weights + weights
        scratch += [vm((TOK, TOK), BF), vm((2, EP, 8, TOK), jnp.int32), vm((2, EP, 8, TOK), F32), vm((2, 8, TOK), jnp.int32)]
        scratch += [vm((2, TOK, EP * TOK), BF)]
        scratch += [vm((E_LOC, EP * CAP, D), BF)] * 3
        scratch += [vm((E_LOC, TILES, EP * CAP, 2 * LANES), F32), vm((E_LOC, EP * CAP, FF), BF), vm((E_LOC, TILES, EP * CAP, 2 * LANES), BF)]
        scratch += [spread_buf, vm((TOK, D), F32), vm((TOK, D), F32)]
        scratch += list(parts) + [dense, dense]
        scratch += [dma((12,)), dma, dma((EP - 1,)), dma((2,)), dma((2, EP - 1, 2)), dma, dma((EP - 1, 2)),
                    dma((3,)), dma((2, 3)), dma((2,)), dma((2,))]
        results = pl.pallas_call(
            kernel,
            out_shape=(vm((TOK, D), BF),) + got + (vm((2, 32, D), BF),),
            in_specs=[hbm] * 14,
            out_specs=(on_chip,) * 5,
            scratch_shapes=scratch,
            name='moe_backward',
            compiler_params=pltpu.CompilerParams(collective_id=0, has_side_effects=True, vmem_limit_bytes=VMEM_LIMIT),
        )(tokens, dy_out, route_idx1.T, route_idx2.T, route_gate1.T, route_gate2.T,
          dense_w1, w_gate1, w_up1, w_down1, dense_w2, w_gate2, w_up2, w_down2)
        return pl.pallas_call(
            finish,
            out_shape=(sds(TOK, D),) + grads + grads,
            in_specs=[on_chip] * 5,
            out_specs=(hbm,) * 9,
            scratch_shapes=[dma((9,))],
            name='finish',
            compiler_params=pltpu.CompilerParams(vmem_limit_bytes=16 * 1024 * 1024),
        )(*[pltpu.with_memory_space_constraint(r, pltpu.VMEM) for r in results])

    return jax.shard_map(local_step, mesh=mesh, in_specs=(tok_spec, tok_spec) + layer_specs + layer_specs,
                         out_specs=(tok_spec,) + grad_specs + grad_specs, check_vma=False)
```

```python
import jax
import jax.numpy as jnp
from jax import lax
from jax.experimental import pallas as pl
from jax.experimental.pallas import tpu as pltpu
from jax.sharding import PartitionSpec as P

MESH = pl.DeviceIdType.MESH
BF = jnp.bfloat16
F32 = jnp.float32
NN = ((1,), (0,))
NT = ((1,), (1,))
TN = ((0,), (0,))
EP = 4
DP = 2
E_LOC = 2
TOK = 512
CAP = 256
D = 256
FF = 896
LANES = 128
TILES = FF // LANES
VMEM_LIMIT = 60 * 1024 * 1024
X_IN, DY, Y_ONE, GM = range(4)
O_ONE, GR_TWO, GR_ONE = range(3)


def dot(a, b, dims=NN):
    return lax.dot_general(a, b, (dims, ((), ())), preferred_element_type=F32)


def place(k):
    return k + 3 * ((k + 3) // 4)


def unit(i):
    q = i // 2
    mid = (q + 1) // 2 % 2
    return mid * (1 + i % 2) + (1 - mid) * q, mid * (q - 1) + (1 - mid) * (i % 2)


def onehot(key_row):
    rows = lax.broadcasted_iota(jnp.int32, (CAP, TOK), 0)
    return jnp.where(rows == key_row, 1.0, 0.0).astype(BF)


def gate_column(key_row, gate_row):
    rows = lax.broadcasted_iota(jnp.int32, (CAP, TOK), 0)
    return jnp.sum(jnp.where(rows == key_row, gate_row, 0.0), axis=1, keepdims=True)


def kernel(tokens, dy, idx1, idx2, gate1, gate2, m1, g1, u1, w1, m2, g2, u2, w2,
           dx_out, got_g, got_u, got_w, dense_sum,
           ibuf, gbuf, rt, xin, dyb, yb, gmb, oret, grt2, grt1,
           vm1, vgu1, vw1, vm2, vgu2, vw2,
           tri, keys, gates, keyj, picks, x1, x2, gout, ab1, hb, gab, ub, p0, p1,
           wg, wu, wd, dpart, dense_got,
           loc_sem, rt_send, rt_recv, ag_send, ag_recv, ret_send, ret_recv, dp_send, dp_recv, all_send, all_recv):
    me = lax.axis_index('ep')
    dp = lax.axis_index('dp')
    flat = dp * EP + me
    other = 1 - dp

    barrier = pltpu.get_barrier_semaphore()
    def partner(k):
        return (me // 2 + k // 2) % 2 * 2 + (me + k) % 2

    for k in (1, 2):
        pl.semaphore_signal(barrier, inc=1, device_id={'ep': partner(k)}, device_id_type=MESH)
    pl.semaphore_signal(barrier, inc=1, device_id={'dp': other}, device_id_type=MESH)

    small = [(idx1, ibuf.at[0]), (idx2, ibuf.at[1]), (gate1, gbuf.at[0]), (gate2, gbuf.at[1]), (tokens, xin.at[0]), (dy, dyb.at[0])]
    small = [pltpu.make_async_copy(src, dst, loc_sem.at[n]) for n, (src, dst) in enumerate(small)]
    for copy in small:
        copy.start()

    def weight_copies(l, m, g, u, w, vm, vgu, vw):
        base = len(small) + 3 * l
        copies = [pltpu.make_async_copy(m, vm, loc_sem.at[base]), pltpu.make_async_copy(w, vw, loc_sem.at[base + 1])]
        for n in range(TILES):
            cols = pl.ds(n * LANES, LANES)
            for src, lanes in ((g, pl.ds(0, LANES)), (u, pl.ds(LANES, LANES))):
                copies.append(pltpu.make_async_copy(src.at[:, :, cols], vgu.at[:, n, :, lanes], loc_sem.at[base + 2]))
        whole = pltpu.make_async_copy(vgu, vgu, loc_sem.at[base + 2])
        return copies, copies[:2] + [whole]

    starts_one, waits_one = weight_copies(0, m1, g1, u1, w1, vm1, vgu1, vw1)
    starts_two, waits_two = weight_copies(1, m2, g2, u2, w2, vm2, vgu2, vw2)
    for copy in starts_one:
        copy.start()

    for copy in small[:4]:
        copy.wait()
    rt[0] = jnp.concatenate([ibuf[0].astype(F32), ibuf[1].astype(F32), gbuf[0], gbuf[1]], axis=0)
    small[4].wait()
    pl.semaphore_wait(barrier, 3)

    def remote(src, dst, send, recv, k):
        return pltpu.make_async_remote_copy(src_ref=src, dst_ref=dst, send_sem=send, recv_sem=recv,
                                            device_id={'ep': partner(k)}, device_id_type=MESH)

    def tell(k):
        return remote(rt.at[0], rt.at[k], rt_send, rt_recv.at[k - 1], k)

    def lane(phase):
        return 1 if phase == DY else 0

    def all_sent(buf, sem):
        remote(buf.at[pl.ds(1, EP - 1)], buf.at[pl.ds(1, EP - 1)], sem, sem, 1).wait_send()

    def half(h):
        return pl.ds(h * CAP, CAP)

    def ship(phase, buf, k, piece):
        rows = half(piece if k == 1 else 1 - piece)
        return remote(buf.at[0, rows], buf.at[k, rows], ag_send.at[lane(phase)], ag_recv.at[lane(phase), k - 1, piece], k)

    def relay(phase, buf, via):
        rows = half(via - 1)
        return remote(buf.at[via, rows], buf.at[3, rows], ag_send.at[lane(phase)], ag_recv.at[lane(phase), 2, via - 1], 3 - via)

    def spread(phase, buf):
        for piece in range(2):
            for k in (1, 2):
                ship(phase, buf, k, piece).start()

    def pass_on(phase, buf):
        for via in (1, 2):
            ship(phase, buf, via, 0).wait_recv()
            relay(phase, buf, via).start()

    def arrive(phase, buf, k):
        if k < 3:
            ship(phase, buf, k, 1).wait_recv()
        else:
            for via in (1, 2):
                relay(phase, buf, via).wait_recv()

    def giveback(phase, buf, k, el):
        rows = pl.ds(pl.multiple_of(el * CAP, CAP), CAP)
        return remote(buf.at[k, rows], buf.at[k + 3, rows], ret_send, ret_recv.at[k - 1, el], k)

    for k in (1, 2):
        tell(k).start()

    @pl.when(dp == 1)
    def _():
        small[5].wait()
        spread(DY, dyb)

    spread(X_IN, xin)
    for copy in starts_two:
        copy.start()

    tri[...] = jnp.where(lax.broadcasted_iota(jnp.int32, (TOK, TOK), 0) < lax.broadcasted_iota(jnp.int32, (TOK, TOK), 1), 1.0, 0.0).astype(BF)
    expert = lax.broadcasted_iota(jnp.int32, (E_LOC * EP, TOK), 0).astype(F32)

    def make_keys(k):
        info = rt[k]
        for l in range(2):
            hit0 = info[2 * l:2 * l + 1] == expert
            hit1 = info[2 * l + 1:2 * l + 2] == expert
            both = jnp.where(hit0, 1.0, jnp.where(hit1, 1.0, 0.0))
            rank = dot(both.astype(BF), tri[...]).astype(jnp.int32)
            keys[l, k] = jnp.where(both > 0.5, rank, -1)
            gates[l, k] = jnp.where(hit0, info[4 + 2 * l:5 + 2 * l], jnp.where(hit1, info[5 + 2 * l:6 + 2 * l], 0.0))
        return info

    info = make_keys(0)
    for j in range(2):
        keyj[j] = jnp.where(info[j:j + 1] == expert, keys[0, 0], -1)
    for copy in waits_one:
        copy.wait()

    def build_picks(*sources):
        slots = lax.broadcasted_iota(jnp.int32, (TOK, CAP), 1)
        for j, source in enumerate(sources):
            rows = [source[pl.ds(partner(k) * E_LOC + el, 1), :] for k in range(EP) for el in range(E_LOC)]
            cols = jnp.transpose(jnp.concatenate(rows, axis=0))
            for r in range(EP * E_LOC):
                picks[j, :, r * CAP:(r + 1) * CAP] = jnp.where(slots == cols[:, r:r + 1], 1.0, 0.0).astype(BF)

    def picked(j, ret, last):
        if last:
            rows = slice((last - 1) * CAP, last * CAP)
            return dot(picks[j, :, 3 * TOK + (last - 1) * CAP:3 * TOK + last * CAP], ret[6, rows])
        return dot(picks[j, :, :TOK], ret[0]) + dot(picks[j, :, TOK:3 * TOK], ret[4:6].reshape(2 * TOK, D))

    def silu_parts(a):
        sig = 0.5 * jnp.tanh(0.5 * a) + 0.5
        return sig, a * sig

    def groups():
        return [range(n, min(n + 2, TILES)) for n in range(0, TILES, 2)]

    def mixed(x, m):
        return (x.astype(F32) + dot(x, m[...])).astype(BF)

    def near_or_far(b):
        return ((b == 1, 1), (b == 1, 2), (b == 3, 3))

    def forward_one(b, carry):
        @pl.when(b == 0)
        def _():
            ub[0] = mixed(xin[0], vm1)

        @pl.when(b == 1)
        def _():
            build_picks(keyj.at[0], keyj.at[1])

            @pl.when(dp == 1)
            def _():
                pass_on(DY, dyb)

            tell(1).wait_recv()
            remote(rt.at[1], rt.at[3], rt_send, rt_recv.at[2], 2).start()
            pass_on(X_IN, xin)

        for ready, src in near_or_far(b):
            @pl.when(ready)
            def _():
                if src > 1:
                    tell(src).wait_recv()
                make_keys(src)
                arrive(X_IN, xin, src)
                ub[src] = mixed(xin[src], vm1)

        for k, el in (unit(2 * b), unit(2 * b + 1)):
            rows = pl.ds(pl.multiple_of(k * CAP, CAP), CAP)
            key = keys[0, k, pl.ds(me * E_LOC + el, 1), :]
            x = dot(onehot(key), ub[k]).astype(BF)
            x1[el, rows] = x
            out = jnp.zeros((CAP, D), F32)
            for group in groups():
                h = []
                for n in group:
                    ab = dot(x, vgu1[el, n])
                    ab1[el, n, rows] = ab
                    h.append((silu_parts(ab[:, :LANES])[1] * ab[:, LANES:]).astype(BF))
                out += dot(jnp.concatenate(h, axis=1), vw1[el, group[0] * LANES:(group[-1] + 1) * LANES])
            oret[k, pl.ds(pl.multiple_of(el * CAP, CAP), CAP)] = out.astype(BF)

        returns(b, O_ONE, oret)
        return carry

    def returns(b, phase, ret):
        @pl.when(b > 0)
        def _():
            for k, el in (unit(2 * b), unit(2 * b + 1)):
                giveback(phase, ret, k, el).start()

    lax.fori_loop(0, EP, forward_one, 0)

    @pl.when(dp == 0)
    def _():
        small[5].wait()
        spread(DY, dyb)

    for copy in waits_two:
        copy.wait()

    def collect(phase, ret, ks, els=range(E_LOC)):
        for k in ks:
            for el in els:
                giveback(phase, ret, k, el).wait_recv()

    collect(O_ONE, oret, (1, 2))
    p0[...] = picked(0, oret, 0)
    p1[...] = picked(1, oret, 0)
    gcol0 = jnp.transpose(jnp.broadcast_to(rt[0, 4:5], (8, TOK)))[:, :1]
    gcol1 = jnp.transpose(jnp.broadcast_to(rt[0, 5:6], (8, TOK)))[:, :1]
    collect(O_ONE, oret, (3,), (0,))
    p0[...] += picked(0, oret, 1)
    p1[...] += picked(1, oret, 1)
    collect(O_ONE, oret, (3,), (1,))
    out0 = p0[...] + picked(0, oret, 2)
    out1 = p1[...] + picked(1, oret, 2)
    yb[0] = (ub[0].astype(F32) + (gcol0 * out0 + gcol1 * out1)).astype(BF)
    @pl.when(dp == 1)
    def _():
        pl.delay(1800)

    all_sent(xin, ag_send.at[0])
    spread(Y_ONE, yb)

    def expert_backward(k, el, first, vgu, vw, ret):
        rows = pl.ds(pl.multiple_of(k * CAP, CAP), CAP)
        go = gout[el, rows]
        back = jnp.zeros((CAP, D), F32)
        for group in groups():
            cols = slice(group[0] * LANES, (group[-1] + 1) * LANES)
            grad_h = dot(go, vw[el, cols], NT).astype(BF).astype(F32)
            for n in group:
                ab = first(n)
                a, b = ab[:, :LANES], ab[:, LANES:]
                dh = grad_h[:, (n - group[0]) * LANES:(n - group[0] + 1) * LANES]
                sig, s = silu_parts(a)
                hb[el, rows, n * LANES:(n + 1) * LANES] = (s * b).astype(BF)
                grad_a = (dh * b * (sig + s * (1.0 - sig))).astype(BF)
                grad_b = (dh * s).astype(BF)
                grads = jnp.concatenate([grad_a, grad_b], axis=1)
                gab[el, n, rows] = grads
                back += dot(grads, vgu[el, n], NT)
        ret[k, pl.ds(pl.multiple_of(el * CAP, CAP), CAP)] = back.astype(BF)

    all_sent(oret, ret_send)

    def layer_two(b, carry):
        @pl.when(b == 0)
        def _():
            ub[0] = mixed(yb[0], vm2)

        @pl.when(b == 1)
        def _():
            build_picks(keys.at[1, 0])

            @pl.when(dp == 0)
            def _():
                pass_on(DY, dyb)

            pass_on(Y_ONE, yb)

        for ready, src in near_or_far(b):
            @pl.when(ready)
            def _():
                arrive(DY, dyb, src)
                arrive(Y_ONE, yb, src)
                ub[src] = mixed(yb[src], vm2)

        for k, el in (unit(2 * b), unit(2 * b + 1)):
            rows = pl.ds(pl.multiple_of(k * CAP, CAP), CAP)
            e = pl.ds(me * E_LOC + el, 1)
            key = keys[1, k, e, :]
            pick = onehot(key)
            x = dot(pick, ub[k]).astype(BF)
            x2[el, rows] = x
            gout[el, rows] = (dot(pick, dyb[k]) * gate_column(key, gates[1, k, e, :])).astype(BF)
            expert_backward(k, el, lambda n: dot(x, vgu2[el, n]), vgu2, vw2, grt2)

        returns(b, GR_TWO, grt2)
        return carry

    lax.fori_loop(0, EP, layer_two, 0)

    stacks = ((wg, got_g), (wu, got_u), (wd, got_w))

    def pairs(l):
        return [pltpu.make_async_remote_copy(src_ref=part.at[l, other], dst_ref=got.at[l], send_sem=dp_send.at[n],
                                             recv_sem=dp_recv.at[l, n], device_id={'dp': other}, device_id_type=MESH)
                for n, (part, got) in enumerate(stacks)]

    def weight_grads(l, x_all, el):
        half_d = D // DP
        x = x_all[el]
        down = dot(hb[el], gout[el], TN).astype(BF)
        for d in range(DP):
            wd[l, d, el] = down[:, d * half_d:(d + 1) * half_d]

        for n in range(TILES):
            cols = slice(n * LANES, (n + 1) * LANES)
            both = dot(x, gab[el, n], TN).astype(BF)
            for d in range(DP):
                rows = slice(d * half_d, (d + 1) * half_d)
                wg[l, d, el, :, cols] = both[rows, :LANES]
                wu[l, d, el, :, cols] = both[rows, LANES:]

    def send_weight_grads(l):
        if l == 0:
            for copy in pairs(1):
                copy.wait_send()
        for copy in pairs(l):
            copy.start()

    weight_grads(1, x2, 0)

    def backward_combine(phase, ret, grad_y):
        collect(phase, ret, (1, 2))
        p0[...] = picked(0, ret, 0)
        collect(phase, ret, (3,), (0,))
        p0[...] += picked(0, ret, 1)
        collect(phase, ret, (3,), (1,))
        return (grad_y.astype(F32) + (p0[...] + picked(0, ret, 2))).astype(BF)

    def grad_input(grad_mixed, m):
        return (grad_mixed.astype(F32) + dot(grad_mixed, m[...], NT)).astype(BF)

    def dense_copies(l):
        copies = []
        for r in range(1, EP * DP):
            peer = (flat + r) % (EP * DP)
            copies.append(pltpu.make_async_remote_copy(
                src_ref=dpart.at[l, peer], dst_ref=dense_got.at[l, r], send_sem=all_send.at[l], recv_sem=all_recv.at[l],
                device_id={'ep': peer % EP, 'dp': peer // EP}, device_id_type=MESH))
        return copies

    def dense_grad(l, x, grad_mixed):
        part = dot(x, grad_mixed, TN).astype(BF)
        for q in range(EP * DP):
            dpart[l, q] = part[q * 32:(q + 1) * 32]
        for copy in dense_copies(l):
            copy.start()

    grad_mixed = backward_combine(GR_TWO, grt2, dyb[0])
    gmb[0] = grad_input(grad_mixed, vm2)
    all_sent(yb, ag_send.at[0])
    spread(GM, gmb)
    weight_grads(1, x2, 1)
    send_weight_grads(1)
    dense_grad(1, yb[0], grad_mixed)

    all_sent(grt2, ret_send)

    def backward_one(b, carry):
        @pl.when(b == 0)
        def _():
            build_picks(keys.at[0, 0])
            pass_on(GM, gmb)

        for ready, src in near_or_far(b):
            @pl.when(ready)
            def _():
                arrive(GM, gmb, src)

        for k, el in (unit(2 * b), unit(2 * b + 1)):
            rows = pl.ds(pl.multiple_of(k * CAP, CAP), CAP)
            e = pl.ds(me * E_LOC + el, 1)
            key = keys[0, k, e, :]
            gout[el, rows] = (dot(onehot(key), gmb[k]) * gate_column(key, gates[0, k, e, :])).astype(BF)
            expert_backward(k, el, lambda n: ab1[el, n, rows], vgu1, vw1, grt1)

        returns(b, GR_ONE, grt1)
        return carry

    lax.fori_loop(0, EP, backward_one, 0)
    weight_grads(0, x1, 0)
    weight_grads(0, x1, 1)
    send_weight_grads(0)
    grad_mixed = backward_combine(GR_ONE, grt1, gmb[0])
    dense_grad(0, xin[0], grad_mixed)
    dx_out[...] = grad_input(grad_mixed, vm1)

    all_sent(rt, rt_send)
    all_sent(dyb, ag_send.at[1])
    all_sent(gmb, ag_send.at[0])
    all_sent(grt1, ret_send)
    for copy in pairs(1):
        copy.wait_recv()
    for copy in pairs(0):
        copy.wait()
    for l in range(2):
        for part, got in stacks:
            got[l] = (part[l, dp].astype(F32) + got[l].astype(F32)).astype(BF)
    for l in range(2):
        whole = pl.ds(1, EP * DP - 1)
        pltpu.make_async_remote_copy(src_ref=dpart.at[l, whole], dst_ref=dense_got.at[l, whole], send_sem=all_send.at[l], recv_sem=all_recv.at[l],
                                     device_id={'dp': other}, device_id_type=MESH).wait()
        total = dpart[l, flat].astype(F32)
        for r in range(1, EP * DP):
            total += dense_got[l, r].astype(F32)
        dense_sum[l] = total.astype(BF)


def finish(dx, got_g, got_u, got_w, dense_sum, dx_out, gd1, gg1, gu1, gw1, gd2, gg2, gu2, gw2, out_sem):
    moves = [(got_g.at[0], gg1), (got_u.at[0], gu1), (got_w.at[0], gw1), (got_g.at[1], gg2), (got_u.at[1], gu2), (got_w.at[1], gw2),
             (dx, dx_out), (dense_sum.at[0], gd1), (dense_sum.at[1], gd2)]
    moves = [pltpu.make_async_copy(src, dst, out_sem.at[n]) for n, (src, dst) in enumerate(moves)]
    for copy in moves:
        copy.start()
    for copy in moves:
        copy.wait()


def solution(mesh):
    tok_spec = P(('dp', 'ep'), None)
    exp_spec = P('ep', None, None)
    layer_specs = (P(None, None), tok_spec, tok_spec, exp_spec, exp_spec, exp_spec)
    grad_specs = (P(('dp', 'ep'), None), P('ep', 'dp', None), P('ep', 'dp', None), P('ep', None, 'dp'))

    def local_step(tokens, dy_out, dense_w1, route_idx1, route_gate1, w_gate1, w_up1, w_down1, dense_w2, route_idx2, route_gate2, w_gate2, w_up2, w_down2):
        hbm = pl.BlockSpec(memory_space=pl.ANY)
        half = D // DP

        def sds(*shape):
            return jax.ShapeDtypeStruct(shape, BF)

        grads = (sds(32, D), sds(E_LOC, half, FF), sds(E_LOC, half, FF), sds(E_LOC, FF, half))
        vm = pltpu.VMEM
        got = (vm((2, E_LOC, half, FF), BF), vm((2, E_LOC, half, FF), BF), vm((2, E_LOC, FF, half), BF))
        parts = (vm((2, DP, E_LOC, half, FF), BF), vm((2, DP, E_LOC, half, FF), BF), vm((2, DP, E_LOC, FF, half), BF))
        dense = vm((2, EP * DP, 32, D), BF)
        on_chip = pl.BlockSpec(memory_space=pltpu.VMEM)
        dma = pltpu.SemaphoreType.DMA
        weights = [vm((D, D), BF), vm((E_LOC, TILES, D, 2 * LANES), BF), vm((E_LOC, FF, D), BF)]
        spread_buf = vm((EP, TOK, D), BF)
        ret_buf = vm((2 * EP - 1, TOK, D), BF)
        scratch = [vm((2, 2, TOK), jnp.int32), vm((2, 2, TOK), F32)]
        scratch += [vm((EP, 8, TOK), F32), spread_buf, spread_buf, spread_buf, spread_buf, ret_buf, ret_buf, ret_buf]
        scratch += weights + weights
        scratch += [vm((TOK, TOK), BF), vm((2, EP, 8, TOK), jnp.int32), vm((2, EP, 8, TOK), F32), vm((2, 8, TOK), jnp.int32)]
        scratch += [vm((2, TOK, EP * TOK), BF)]
        scratch += [vm((E_LOC, EP * CAP, D), BF)] * 3
        scratch += [vm((E_LOC, TILES, EP * CAP, 2 * LANES), F32), vm((E_LOC, EP * CAP, FF), BF), vm((E_LOC, TILES, EP * CAP, 2 * LANES), BF)]
        scratch += [spread_buf, vm((TOK, D), F32), vm((TOK, D), F32)]
        scratch += list(parts) + [dense, dense]
        scratch += [dma((12,)), dma, dma((EP - 1,)), dma((2,)), dma((2, EP - 1, 2)), dma, dma((EP - 1, 2)),
                    dma((3,)), dma((2, 3)), dma((2,)), dma((2,))]
        results = pl.pallas_call(
            kernel,
            out_shape=(vm((TOK, D), BF),) + got + (vm((2, 32, D), BF),),
            in_specs=[hbm] * 14,
            out_specs=(on_chip,) * 5,
            scratch_shapes=scratch,
            name='moe_backward',
            compiler_params=pltpu.CompilerParams(collective_id=0, has_side_effects=True, vmem_limit_bytes=VMEM_LIMIT),
        )(tokens, dy_out, route_idx1.T, route_idx2.T, route_gate1.T, route_gate2.T,
          dense_w1, w_gate1, w_up1, w_down1, dense_w2, w_gate2, w_up2, w_down2)
        return pl.pallas_call(
            finish,
            out_shape=(sds(TOK, D),) + grads + grads,
            in_specs=[on_chip] * 5,
            out_specs=(hbm,) * 9,
            scratch_shapes=[dma((9,))],
            name='finish',
            compiler_params=pltpu.CompilerParams(vmem_limit_bytes=16 * 1024 * 1024),
        )(*[pltpu.with_memory_space_constraint(r, pltpu.VMEM) for r in results])

    return jax.shard_map(local_step, mesh=mesh, in_specs=(tok_spec, tok_spec) + layer_specs + layer_specs,
                         out_specs=(tok_spec,) + grad_specs + grad_specs, check_vma=False)
```

```python
import jax
import jax.numpy as jnp
from jax import lax
from jax.experimental import pallas as pl
from jax.experimental.pallas import tpu as pltpu
from jax.sharding import PartitionSpec as P

MESH = pl.DeviceIdType.MESH
BF = jnp.bfloat16
F32 = jnp.float32
NN = ((1,), (0,))
NT = ((1,), (1,))
TN = ((0,), (0,))
EP = 4
DP = 2
E_LOC = 2
TOK = 512
CAP = 256
D = 256
FF = 896
LANES = 128
TILES = FF // LANES
VMEM_LIMIT = 60 * 1024 * 1024
X_IN, DY, Y_ONE, GM = range(4)
O_ONE, GR_TWO, GR_ONE = range(3)


def dot(a, b, dims=NN):
    return lax.dot_general(a, b, (dims, ((), ())), preferred_element_type=F32)


def place(k):
    return k + 3 * ((k + 3) // 4)


def unit(i):
    q = i // 2
    mid = (q + 1) // 2 % 2
    return mid * (1 + i % 2) + (1 - mid) * q, mid * (q - 1) + (1 - mid) * (i % 2)


def onehot(key_row):
    rows = lax.broadcasted_iota(jnp.int32, (CAP, TOK), 0)
    return jnp.where(rows == key_row, 1.0, 0.0).astype(BF)


def gate_column(key_row, gate_row):
    rows = lax.broadcasted_iota(jnp.int32, (CAP, TOK), 0)
    return jnp.sum(jnp.where(rows == key_row, gate_row, 0.0), axis=1, keepdims=True)


def kernel(tokens, dy, idx1, idx2, gate1, gate2, m1, g1, u1, w1, m2, g2, u2, w2,
           dx_out, got_g, got_u, got_w, dense_sum,
           ibuf, gbuf, rt, xin, dyb, yb, gmb, oret, grt2, grt1,
           vm1, vgu1, vw1, vm2, vgu2, vw2,
           tri, keys, gates, keyj, picks, x1, x2, gout, ab1, hb, gab, ub, p0, p1,
           wg, wu, wd, dpart, dense_got,
           loc_sem, rt_send, rt_recv, ag_send, ag_recv, ret_send, ret_recv, dp_send, dp_recv, all_send, all_recv):
    me = lax.axis_index('ep')
    dp = lax.axis_index('dp')
    flat = dp * EP + me
    other = 1 - dp

    barrier = pltpu.get_barrier_semaphore()
    def partner(k):
        return (me // 2 + k // 2) % 2 * 2 + (me + k) % 2

    for k in (1, 2):
        pl.semaphore_signal(barrier, inc=1, device_id={'ep': partner(k)}, device_id_type=MESH)
    pl.semaphore_signal(barrier, inc=1, device_id={'dp': other}, device_id_type=MESH)

    small = [(idx1, ibuf.at[0]), (idx2, ibuf.at[1]), (gate1, gbuf.at[0]), (gate2, gbuf.at[1]), (tokens, xin.at[0]), (dy, dyb.at[0])]
    small = [pltpu.make_async_copy(src, dst, loc_sem.at[n]) for n, (src, dst) in enumerate(small)]
    for copy in small:
        copy.start()

    def weight_copies(l, m, g, u, w, vm, vgu, vw):
        base = len(small) + 3 * l
        copies = [pltpu.make_async_copy(m, vm, loc_sem.at[base]), pltpu.make_async_copy(w, vw, loc_sem.at[base + 1])]
        for n in range(TILES):
            cols = pl.ds(n * LANES, LANES)
            for src, lanes in ((g, pl.ds(0, LANES)), (u, pl.ds(LANES, LANES))):
                copies.append(pltpu.make_async_copy(src.at[:, :, cols], vgu.at[:, n, :, lanes], loc_sem.at[base + 2]))
        whole = pltpu.make_async_copy(vgu, vgu, loc_sem.at[base + 2])
        return copies, copies[:2] + [whole]

    starts_one, waits_one = weight_copies(0, m1, g1, u1, w1, vm1, vgu1, vw1)
    starts_two, waits_two = weight_copies(1, m2, g2, u2, w2, vm2, vgu2, vw2)
    for copy in starts_one:
        copy.start()

    for copy in small[:4]:
        copy.wait()
    rt[0] = jnp.concatenate([ibuf[0].astype(F32), ibuf[1].astype(F32), gbuf[0], gbuf[1]], axis=0)
    small[4].wait()
    pl.semaphore_wait(barrier, 3)

    def remote(src, dst, send, recv, k):
        return pltpu.make_async_remote_copy(src_ref=src, dst_ref=dst, send_sem=send, recv_sem=recv,
                                            device_id={'ep': partner(k)}, device_id_type=MESH)

    def tell(k):
        return remote(rt.at[0], rt.at[k], rt_send, rt_recv.at[k - 1], k)

    def lane(phase):
        return 1 if phase == DY else 0

    def all_sent(buf, sem):
        remote(buf.at[pl.ds(1, EP - 1)], buf.at[pl.ds(1, EP - 1)], sem, sem, 1).wait_send()

    def half(h):
        return pl.ds(h * CAP, CAP)

    def ship(phase, buf, k, piece):
        rows = half(piece if k == 1 else 1 - piece)
        return remote(buf.at[0, rows], buf.at[k, rows], ag_send.at[lane(phase)], ag_recv.at[lane(phase), k - 1, piece], k)

    def relay(phase, buf, via):
        rows = half(via - 1)
        return remote(buf.at[via, rows], buf.at[3, rows], ag_send.at[lane(phase)], ag_recv.at[lane(phase), 2, via - 1], 3 - via)

    def spread(phase, buf):
        for piece in range(2):
            for k in (1, 2):
                ship(phase, buf, k, piece).start()

    def pass_on(phase, buf):
        for via in (1, 2):
            ship(phase, buf, via, 0).wait_recv()
            relay(phase, buf, via).start()

    def arrive(phase, buf, k):
        if k < 3:
            ship(phase, buf, k, 1).wait_recv()
        else:
            for via in (1, 2):
                relay(phase, buf, via).wait_recv()

    def giveback(phase, buf, k, el):
        rows = pl.ds(pl.multiple_of(el * CAP, CAP), CAP)
        return remote(buf.at[k, rows], buf.at[k + 3, rows], ret_send, ret_recv.at[k - 1, el], k)

    for k in (1, 2):
        tell(k).start()

    @pl.when(dp == 1)
    def _():
        small[5].wait()
        spread(DY, dyb)

    spread(X_IN, xin)
    for copy in starts_two:
        copy.start()

    tri[...] = jnp.where(lax.broadcasted_iota(jnp.int32, (TOK, TOK), 0) < lax.broadcasted_iota(jnp.int32, (TOK, TOK), 1), 1.0, 0.0).astype(BF)
    expert = lax.broadcasted_iota(jnp.int32, (E_LOC * EP, TOK), 0).astype(F32)

    def make_keys(k):
        info = rt[k]
        for l in range(2):
            hit0 = info[2 * l:2 * l + 1] == expert
            hit1 = info[2 * l + 1:2 * l + 2] == expert
            both = jnp.where(hit0, 1.0, jnp.where(hit1, 1.0, 0.0))
            rank = dot(both.astype(BF), tri[...]).astype(jnp.int32)
            keys[l, k] = jnp.where(both > 0.5, rank, -1)
            gates[l, k] = jnp.where(hit0, info[4 + 2 * l:5 + 2 * l], jnp.where(hit1, info[5 + 2 * l:6 + 2 * l], 0.0))
        return info

    info = make_keys(0)
    for j in range(2):
        keyj[j] = jnp.where(info[j:j + 1] == expert, keys[0, 0], -1)
    for copy in waits_one:
        copy.wait()

    def build_picks(*sources):
        slots = lax.broadcasted_iota(jnp.int32, (TOK, CAP), 1)
        for j, source in enumerate(sources):
            rows = [source[pl.ds(partner(k) * E_LOC + el, 1), :] for k in range(EP) for el in range(E_LOC)]
            cols = jnp.transpose(jnp.concatenate(rows, axis=0))
            for r in range(EP * E_LOC):
                picks[j, :, r * CAP:(r + 1) * CAP] = jnp.where(slots == cols[:, r:r + 1], 1.0, 0.0).astype(BF)

    def picked(j, ret, last):
        if last:
            rows = slice((last - 1) * CAP, last * CAP)
            return dot(picks[j, :, 3 * TOK + (last - 1) * CAP:3 * TOK + last * CAP], ret[6, rows])
        return dot(picks[j, :, TOK:3 * TOK], ret[4:6].reshape(2 * TOK, D))

    def picked_own(j, ret):
        return dot(picks[j, :, :TOK], ret[0])

    def silu_parts(a):
        sig = 0.5 * jnp.tanh(0.5 * a) + 0.5
        return sig, a * sig

    def groups():
        return [range(n, min(n + 2, TILES)) for n in range(0, TILES, 2)]

    def mixed(x, m):
        return (x.astype(F32) + dot(x, m[...])).astype(BF)

    def near_or_far(b):
        return ((b == 1, 1), (b == 1, 2), (b == 3, 3))

    def forward_one(b, carry):
        @pl.when(b == 0)
        def _():
            ub[0] = mixed(xin[0], vm1)

        @pl.when(b == 1)
        def _():
            build_picks(keyj.at[0], keyj.at[1])

            @pl.when(dp == 1)
            def _():
                pass_on(DY, dyb)

            tell(1).wait_recv()
            remote(rt.at[1], rt.at[3], rt_send, rt_recv.at[2], 2).start()
            pass_on(X_IN, xin)

        for ready, src in near_or_far(b):
            @pl.when(ready)
            def _():
                if src > 1:
                    tell(src).wait_recv()
                make_keys(src)
                arrive(X_IN, xin, src)
                ub[src] = mixed(xin[src], vm1)

        for k, el in (unit(2 * b), unit(2 * b + 1)):
            rows = pl.ds(pl.multiple_of(k * CAP, CAP), CAP)
            key = keys[0, k, pl.ds(me * E_LOC + el, 1), :]
            x = dot(onehot(key), ub[k]).astype(BF)
            x1[el, rows] = x
            out = jnp.zeros((CAP, D), F32)
            for group in groups():
                h = []
                for n in group:
                    ab = dot(x, vgu1[el, n])
                    ab1[el, n, rows] = ab
                    h.append((silu_parts(ab[:, :LANES])[1] * ab[:, LANES:]).astype(BF))
                out += dot(jnp.concatenate(h, axis=1), vw1[el, group[0] * LANES:(group[-1] + 1) * LANES])
            oret[k, pl.ds(pl.multiple_of(el * CAP, CAP), CAP)] = out.astype(BF)

        returns(b, O_ONE, oret)
        return carry

    def returns(b, phase, ret):
        @pl.when(b > 0)
        def _():
            for k, el in (unit(2 * b), unit(2 * b + 1)):
                giveback(phase, ret, k, el).start()

    lax.fori_loop(0, EP, forward_one, 0)

    @pl.when(dp == 0)
    def _():
        small[5].wait()
        spread(DY, dyb)

    for copy in waits_two:
        copy.wait()

    def collect(phase, ret, ks, els=range(E_LOC)):
        for k in ks:
            for el in els:
                giveback(phase, ret, k, el).wait_recv()

    p0[...] = picked_own(0, oret)
    p1[...] = picked_own(1, oret)
    collect(O_ONE, oret, (1, 2))
    p0[...] += picked(0, oret, 0)
    p1[...] += picked(1, oret, 0)
    gcol0 = jnp.transpose(jnp.broadcast_to(rt[0, 4:5], (8, TOK)))[:, :1]
    gcol1 = jnp.transpose(jnp.broadcast_to(rt[0, 5:6], (8, TOK)))[:, :1]
    collect(O_ONE, oret, (3,), (0,))
    p0[...] += picked(0, oret, 1)
    p1[...] += picked(1, oret, 1)
    collect(O_ONE, oret, (3,), (1,))
    out0 = p0[...] + picked(0, oret, 2)
    out1 = p1[...] + picked(1, oret, 2)
    yb[0] = (ub[0].astype(F32) + (gcol0 * out0 + gcol1 * out1)).astype(BF)
    @pl.when(dp == 1)
    def _():
        pl.delay(1800)

    all_sent(xin, ag_send.at[0])
    spread(Y_ONE, yb)

    def expert_backward(k, el, first, vgu, vw, ret):
        rows = pl.ds(pl.multiple_of(k * CAP, CAP), CAP)
        go = gout[el, rows]
        back = jnp.zeros((CAP, D), F32)
        for group in groups():
            cols = slice(group[0] * LANES, (group[-1] + 1) * LANES)
            grad_h = dot(go, vw[el, cols], NT).astype(BF).astype(F32)
            for n in group:
                ab = first(n)
                a, b = ab[:, :LANES], ab[:, LANES:]
                dh = grad_h[:, (n - group[0]) * LANES:(n - group[0] + 1) * LANES]
                sig, s = silu_parts(a)
                hb[el, rows, n * LANES:(n + 1) * LANES] = (s * b).astype(BF)
                grad_a = (dh * b * (sig + s * (1.0 - sig))).astype(BF)
                grad_b = (dh * s).astype(BF)
                grads = jnp.concatenate([grad_a, grad_b], axis=1)
                gab[el, n, rows] = grads
                back += dot(grads, vgu[el, n], NT)
        ret[k, pl.ds(pl.multiple_of(el * CAP, CAP), CAP)] = back.astype(BF)

    all_sent(oret, ret_send)

    def layer_two(b, carry):
        @pl.when(b == 0)
        def _():
            ub[0] = mixed(yb[0], vm2)

        @pl.when(b == 1)
        def _():
            build_picks(keys.at[1, 0])

            @pl.when(dp == 0)
            def _():
                pass_on(DY, dyb)

            pass_on(Y_ONE, yb)

        for ready, src in near_or_far(b):
            @pl.when(ready)
            def _():
                arrive(DY, dyb, src)
                arrive(Y_ONE, yb, src)
                ub[src] = mixed(yb[src], vm2)

        for k, el in (unit(2 * b), unit(2 * b + 1)):
            rows = pl.ds(pl.multiple_of(k * CAP, CAP), CAP)
            e = pl.ds(me * E_LOC + el, 1)
            key = keys[1, k, e, :]
            pick = onehot(key)
            x = dot(pick, ub[k]).astype(BF)
            x2[el, rows] = x
            gout[el, rows] = (dot(pick, dyb[k]) * gate_column(key, gates[1, k, e, :])).astype(BF)
            expert_backward(k, el, lambda n: dot(x, vgu2[el, n]), vgu2, vw2, grt2)

        returns(b, GR_TWO, grt2)
        return carry

    lax.fori_loop(0, EP, layer_two, 0)

    stacks = ((wg, got_g), (wu, got_u), (wd, got_w))

    def pairs(l):
        return [pltpu.make_async_remote_copy(src_ref=part.at[l, other], dst_ref=got.at[l], send_sem=dp_send.at[n],
                                             recv_sem=dp_recv.at[l, n], device_id={'dp': other}, device_id_type=MESH)
                for n, (part, got) in enumerate(stacks)]

    def weight_grads(l, x_all, el):
        half_d = D // DP
        x = x_all[el]
        down = dot(hb[el], gout[el], TN).astype(BF)
        for d in range(DP):
            wd[l, d, el] = down[:, d * half_d:(d + 1) * half_d]

        for n in range(TILES):
            cols = slice(n * LANES, (n + 1) * LANES)
            both = dot(x, gab[el, n], TN).astype(BF)
            for d in range(DP):
                rows = slice(d * half_d, (d + 1) * half_d)
                wg[l, d, el, :, cols] = both[rows, :LANES]
                wu[l, d, el, :, cols] = both[rows, LANES:]

    def send_weight_grads(l):
        if l == 0:
            for copy in pairs(1):
                copy.wait_send()
        for copy in pairs(l):
            copy.start()

    weight_grads(1, x2, 0)

    def backward_combine(phase, ret, grad_y):
        p0[...] = picked_own(0, ret)
        collect(phase, ret, (1, 2))
        p0[...] += picked(0, ret, 0)
        collect(phase, ret, (3,), (0,))
        p0[...] += picked(0, ret, 1)
        collect(phase, ret, (3,), (1,))
        return (grad_y.astype(F32) + (p0[...] + picked(0, ret, 2))).astype(BF)

    def grad_input(grad_mixed, m):
        return (grad_mixed.astype(F32) + dot(grad_mixed, m[...], NT)).astype(BF)

    def dense_copies(l):
        copies = []
        for r in range(1, EP * DP):
            peer = (flat + r) % (EP * DP)
            copies.append(pltpu.make_async_remote_copy(
                src_ref=dpart.at[l, peer], dst_ref=dense_got.at[l, r], send_sem=all_send.at[l], recv_sem=all_recv.at[l],
                device_id={'ep': peer % EP, 'dp': peer // EP}, device_id_type=MESH))
        return copies

    def dense_grad(l, x, grad_mixed):
        part = dot(x, grad_mixed, TN).astype(BF)
        for q in range(EP * DP):
            dpart[l, q] = part[q * 32:(q + 1) * 32]
        for copy in dense_copies(l):
            copy.start()

    grad_mixed = backward_combine(GR_TWO, grt2, dyb[0])
    gmb[0] = grad_input(grad_mixed, vm2)
    all_sent(yb, ag_send.at[0])
    spread(GM, gmb)
    weight_grads(1, x2, 1)
    send_weight_grads(1)
    dense_grad(1, yb[0], grad_mixed)

    all_sent(grt2, ret_send)

    def backward_one(b, carry):
        @pl.when(b == 0)
        def _():
            build_picks(keys.at[0, 0])
            pass_on(GM, gmb)

        for ready, src in near_or_far(b):
            @pl.when(ready)
            def _():
                arrive(GM, gmb, src)

        for k, el in (unit(2 * b), unit(2 * b + 1)):
            rows = pl.ds(pl.multiple_of(k * CAP, CAP), CAP)
            e = pl.ds(me * E_LOC + el, 1)
            key = keys[0, k, e, :]
            gout[el, rows] = (dot(onehot(key), gmb[k]) * gate_column(key, gates[0, k, e, :])).astype(BF)
            expert_backward(k, el, lambda n: ab1[el, n, rows], vgu1, vw1, grt1)

        returns(b, GR_ONE, grt1)
        return carry

    lax.fori_loop(0, EP, backward_one, 0)
    weight_grads(0, x1, 0)
    weight_grads(0, x1, 1)
    send_weight_grads(0)
    grad_mixed = backward_combine(GR_ONE, grt1, gmb[0])
    dense_grad(0, xin[0], grad_mixed)
    dx_out[...] = grad_input(grad_mixed, vm1)

    all_sent(rt, rt_send)
    all_sent(dyb, ag_send.at[1])
    all_sent(gmb, ag_send.at[0])
    all_sent(grt1, ret_send)
    for copy in pairs(1):
        copy.wait_recv()
    for copy in pairs(0):
        copy.wait()
    for l in range(2):
        for part, got in stacks:
            got[l] = (part[l, dp].astype(F32) + got[l].astype(F32)).astype(BF)
    for l in range(2):
        whole = pl.ds(1, EP * DP - 1)
        pltpu.make_async_remote_copy(src_ref=dpart.at[l, whole], dst_ref=dense_got.at[l, whole], send_sem=all_send.at[l], recv_sem=all_recv.at[l],
                                     device_id={'dp': other}, device_id_type=MESH).wait()
        total = dpart[l, flat].astype(F32)
        for r in range(1, EP * DP):
            total += dense_got[l, r].astype(F32)
        dense_sum[l] = total.astype(BF)


def finish(dx, got_g, got_u, got_w, dense_sum, dx_out, gd1, gg1, gu1, gw1, gd2, gg2, gu2, gw2, out_sem):
    moves = [(got_g.at[0], gg1), (got_u.at[0], gu1), (got_w.at[0], gw1), (got_g.at[1], gg2), (got_u.at[1], gu2), (got_w.at[1], gw2),
             (dx, dx_out), (dense_sum.at[0], gd1), (dense_sum.at[1], gd2)]
    moves = [pltpu.make_async_copy(src, dst, out_sem.at[n]) for n, (src, dst) in enumerate(moves)]
    for copy in moves:
        copy.start()
    for copy in moves:
        copy.wait()


def solution(mesh):
    tok_spec = P(('dp', 'ep'), None)
    exp_spec = P('ep', None, None)
    layer_specs = (P(None, None), tok_spec, tok_spec, exp_spec, exp_spec, exp_spec)
    grad_specs = (P(('dp', 'ep'), None), P('ep', 'dp', None), P('ep', 'dp', None), P('ep', None, 'dp'))

    def local_step(tokens, dy_out, dense_w1, route_idx1, route_gate1, w_gate1, w_up1, w_down1, dense_w2, route_idx2, route_gate2, w_gate2, w_up2, w_down2):
        hbm = pl.BlockSpec(memory_space=pl.ANY)
        half = D // DP

        def sds(*shape):
            return jax.ShapeDtypeStruct(shape, BF)

        grads = (sds(32, D), sds(E_LOC, half, FF), sds(E_LOC, half, FF), sds(E_LOC, FF, half))
        vm = pltpu.VMEM
        got = (vm((2, E_LOC, half, FF), BF), vm((2, E_LOC, half, FF), BF), vm((2, E_LOC, FF, half), BF))
        parts = (vm((2, DP, E_LOC, half, FF), BF), vm((2, DP, E_LOC, half, FF), BF), vm((2, DP, E_LOC, FF, half), BF))
        dense = vm((2, EP * DP, 32, D), BF)
        on_chip = pl.BlockSpec(memory_space=pltpu.VMEM)
        dma = pltpu.SemaphoreType.DMA
        weights = [vm((D, D), BF), vm((E_LOC, TILES, D, 2 * LANES), BF), vm((E_LOC, FF, D), BF)]
        spread_buf = vm((EP, TOK, D), BF)
        ret_buf = vm((2 * EP - 1, TOK, D), BF)
        scratch = [vm((2, 2, TOK), jnp.int32), vm((2, 2, TOK), F32)]
        scratch += [vm((EP, 8, TOK), F32), spread_buf, spread_buf, spread_buf, spread_buf, ret_buf, ret_buf, ret_buf]
        scratch += weights + weights
        scratch += [vm((TOK, TOK), BF), vm((2, EP, 8, TOK), jnp.int32), vm((2, EP, 8, TOK), F32), vm((2, 8, TOK), jnp.int32)]
        scratch += [vm((2, TOK, EP * TOK), BF)]
        scratch += [vm((E_LOC, EP * CAP, D), BF)] * 3
        scratch += [vm((E_LOC, TILES, EP * CAP, 2 * LANES), F32), vm((E_LOC, EP * CAP, FF), BF), vm((E_LOC, TILES, EP * CAP, 2 * LANES), BF)]
        scratch += [spread_buf, vm((TOK, D), F32), vm((TOK, D), F32)]
        scratch += list(parts) + [dense, dense]
        scratch += [dma((12,)), dma, dma((EP - 1,)), dma((2,)), dma((2, EP - 1, 2)), dma, dma((EP - 1, 2)),
                    dma((3,)), dma((2, 3)), dma((2,)), dma((2,))]
        results = pl.pallas_call(
            kernel,
            out_shape=(vm((TOK, D), BF),) + got + (vm((2, 32, D), BF),),
            in_specs=[hbm] * 14,
            out_specs=(on_chip,) * 5,
            scratch_shapes=scratch,
            name='moe_backward',
            compiler_params=pltpu.CompilerParams(collective_id=0, has_side_effects=True, vmem_limit_bytes=VMEM_LIMIT),
        )(tokens, dy_out, route_idx1.T, route_idx2.T, route_gate1.T, route_gate2.T,
          dense_w1, w_gate1, w_up1, w_down1, dense_w2, w_gate2, w_up2, w_down2)
        return pl.pallas_call(
            finish,
            out_shape=(sds(TOK, D),) + grads + grads,
            in_specs=[on_chip] * 5,
            out_specs=(hbm,) * 9,
            scratch_shapes=[dma((9,))],
            name='finish',
            compiler_params=pltpu.CompilerParams(vmem_limit_bytes=16 * 1024 * 1024),
        )(*[pltpu.with_memory_space_constraint(r, pltpu.VMEM) for r in results])

    return jax.shard_map(local_step, mesh=mesh, in_specs=(tok_spec, tok_spec) + layer_specs + layer_specs,
                         out_specs=(tok_spec,) + grad_specs + grad_specs, check_vma=False)
```
